256 devices in a mesh: dp: 8 (over y, core), expert: 32 (over z, x).
Axes of the slice: x: 4, y: 4, z: 8, core: 2. Of those that a mesh axis runs over, the one named last changes fastest.
Arguments:
- tokens: bfloat16 [32768, 1024], P(('dp', 'expert')), may hold values from -6 to 6
- cotangent: bfloat16 [32768, 1024], P(('dp', 'expert')), may hold values from -2 to 2
- expert_ids: int32 [32768, 10], P(('dp', 'expert')), may hold values from 0 to 255, all different within a row; in each aligned block of 128 rows (0 to 127, 128 to 255, ...) at most 6 rows name the same one
- gate_weights: bfloat16 [32768, 10], P(('dp', 'expert')), may hold values from 0.019897461 to 0.29882812
- expert_weights: bfloat16 [256, 3, 1024, 512], P(('dp', 'expert')), may hold values from -0.1875 to 0.1875
- shared_weights: bfloat16 [3, 1024, 512], replicated, may hold values from -0.1875 to 0.1875
Outputs:
- grad_tokens: bfloat16 [32768, 1024], P(('dp', 'expert'))
- grad_gates: bfloat16 [32768, 10], P(('dp', 'expert'))
- grad_experts: bfloat16 [256, 3, 1024, 512], P(('dp', 'expert'))
- grad_shared: float32 [3, 1024, 512], P(None, 'dp')
The draws below stay inside these ranges and needn't reach their ends.
Inputs may be any that keep to these rules, and one draw needn't show every extreme that they name: `expert_ids`: each token names 10 different experts. Among the 128 tokens of one device no expert is named more than 6 times, and in some device's tokens some expert is named exactly 6 times.
All inputs are finite; a program needn't handle non-finite values.
Results may differ from the reference program's by a relative error of at most 0.0052.
Values may be sent and summed in bfloat16 or wider, within the bound.
A program may use at most 128 MiB of HBM per device.

```python
import math
import jax
import jax.numpy as jnp
import numpy as np
from jax import lax

D = 1024
F = 512
F_SH = 512
TOP = 10
TOK_DEV = 128
TOKENS = 32768
EXPERTS = 256
CAP = 6
DEVICES = 256


def levels(own_key, extent, cuts, smallest, largest):
    level = 1.0
    for dim, shards_of in cuts:
        steps = jax.random.uniform(jax.random.fold_in(jax.random.fold_in(own_key, 6), dim), (shards_of,), jnp.float32, smallest / len(cuts), largest / len(cuts))
        level = level * jnp.repeat(jnp.exp(steps), extent[dim] // shards_of).reshape((-1,) + (1,) * (len(extent) - 1 - dim))
    return level


def deal_out(key, own, number, rows, number_of, top, reach, skew):
    order = jax.random.permutation(key, number_of)
    crowded, common = shares(number_of, rows * top, reach, skew, True), shares(number_of, rows * top, reach, skew, False)
    places = jnp.arange(number_of)

    def named(tallies, offset_by):
        used = int((tallies > 0).sum())
        fixed = max(1, used // 4)
        shifted = fixed + (places - fixed + offset_by * (used - fixed)) % max(1, number_of - fixed)
        return jnp.zeros((number_of,), jnp.int32).at[order[jnp.where(places < fixed, places, shifted)]].set(jnp.asarray(tallies, jnp.int32))

    tallies = jnp.where(number % 4 == 0, named(crowded, number // 4), named(common, number - number // 4 - 1))
    mixed = jax.random.permutation(jax.random.fold_in(own, 3), number_of)
    giver, sink = mixed[0:number_of // 2 * 2:2], mixed[1:number_of // 2 * 2:2]
    slack = jnp.minimum(tallies[giver] - 1, reach - tallies[sink]) // 2
    slack = jnp.where((giver == order[0]) | (sink == order[0]) | (tallies[sink] == 0), 0, jnp.maximum(slack, 0))
    shifted = jax.random.randint(jax.random.fold_in(own, 4), (number_of // 2,), 0, 1 << 20) % (slack + 1)
    tallies = tallies.at[giver].add(-shifted).at[sink].add(shifted)
    labels = jnp.searchsorted(jnp.cumsum(tallies), jnp.arange(rows * top), side="right").astype(jnp.int32)
    grid = labels.reshape(top, rows).T
    grid = grid[jax.random.permutation(jax.random.fold_in(own, 1), rows)]
    offset_by = jax.random.randint(jax.random.fold_in(own, 2), (rows, 1), 0, top)
    return jnp.take_along_axis(grid, (jnp.arange(top)[None, :] + offset_by) % top, axis=1)


def shares(amount, total, reach, skew, full):
    weights = [(1 << 20) // math.isqrt(standing ** skew) + 1 for standing in range(1, amount + 1)]
    largest = reach if full else min(reach, max(-(-total // amount), total * weights[0] // sum(weights)))
    least = 1 if total - largest >= amount - 1 else 0
    counts, surplus = [largest] + [least] * (amount - 1), total - largest - least * (amount - 1)
    while surplus > 0:
        candidates = [i for i in range(1, amount) if counts[i] < largest] or [i for i in range(1, amount) if counts[i] < reach]
        mass, budget = sum([weights[i] for i in candidates]), surplus
        for i in candidates:
            addition = min(reach - counts[i], max(1, budget * weights[i] // mass), surplus)
            counts[i] = counts[i] + addition
            surplus = surplus - addition
    return np.array(counts)


def bell_draw(own_key, extent, deviation, limit, cuts=(), kind=jnp.bfloat16):
    array = deviation * jax.random.normal(own_key, extent, jnp.float32)
    if cuts:
        array = array * levels(own_key, extent, cuts, -0.22, 0.18)
    return jnp.clip(array, -limit, limit).astype(kind)


def setup_inputs(seed: int = 0) -> dict:
    key_list = jax.random.split(jax.random.key(seed), 7)
    tokens = bell_draw(key_list[0], (TOKENS, D), 1.0, 6.0, ((0, 256),))
    cotangent = bell_draw(key_list[1], (TOKENS, D), 0.25, 2.0, ((0, 256),))
    expert_ids_keys = jax.random.split(jax.random.fold_in(key_list[2], 1), TOKENS // TOK_DEV)
    expert_ids_turns = jax.random.permutation(jax.random.fold_in(key_list[2], 3), TOKENS // TOK_DEV)
    expert_ids = jax.vmap(lambda own, number: deal_out(jax.random.fold_in(key_list[2], 2), own, number, TOK_DEV, EXPERTS, TOP, CAP, 2))(expert_ids_keys, expert_ids_turns).reshape((TOKENS, TOP))
    gate_weights = jnp.clip(jnp.exp(math.log(0.29882812) - 2.7092764 * jax.random.uniform(key_list[3], (TOKENS, TOP), jnp.float32) ** levels(key_list[3], (TOKENS, TOP), ((0, 256),), -0.2, 0.2)), 0.019897461, 0.29882812).astype(jnp.bfloat16)
    expert_weights = bell_draw(key_list[4], (EXPERTS, 3, D, F), D ** -0.5, 0.1875, ((0, 256),))
    shared_weights = bell_draw(key_list[5], (3, D, F_SH), D ** -0.5, 0.1875)
    return dict(tokens=tokens, cotangent=cotangent, expert_ids=expert_ids, gate_weights=gate_weights, expert_weights=expert_weights, shared_weights=shared_weights)


def silu_parts(pre):
    sigma = jax.nn.sigmoid(pre)
    return pre * sigma, sigma * (1.0 + pre * (1.0 - sigma))


def contract_rows(left, right):
    return jnp.dot(left.T, right, preferred_element_type=jnp.float32)


def expert_grads(inputs, upstream, scales, weight):
    hidden_units = weight.shape[2]
    paired = jnp.concatenate([weight[0], weight[1]], axis=1)
    gate_up = jnp.dot(inputs, paired, preferred_element_type=jnp.float32)
    pre_gate = gate_up[:, :hidden_units]
    pre_up = gate_up[:, hidden_units:]
    back = jnp.dot(upstream, weight[2], preferred_element_type=jnp.float32)
    activated, slope = silu_parts(pre_gate)
    hidden = activated * pre_up
    gate_grad = jnp.sum(hidden * back, axis=1)
    scaled = scales[:, None] * back
    grad_gate_in = (scaled * pre_up * slope).astype(jnp.bfloat16)
    grad_up_in = (scaled * activated).astype(jnp.bfloat16)
    both = jnp.concatenate([grad_gate_in, grad_up_in], axis=1)
    input_grad = jnp.dot(both, paired.T, preferred_element_type=jnp.float32)
    hidden_b = hidden.astype(jnp.bfloat16)
    scaled_up = (scales[:, None] * upstream.astype(jnp.float32)).astype(jnp.bfloat16)
    return input_grad, gate_grad, grad_gate_in, grad_up_in, hidden_b, scaled_up


def weight_terms(inputs, grad_gate_in, grad_up_in, scaled_up, hidden_b):
    return jnp.stack([contract_rows(inputs, grad_gate_in), contract_rows(inputs, grad_up_in),
                      contract_rows(scaled_up, hidden_b)], axis=0)


def reference(tokens, cotangent, expert_ids, gate_weights, expert_weights, shared_weights):
    pair_count = TOKENS * TOP
    row_ids = jnp.arange(TOKENS, dtype=jnp.int32)
    onehot = jnp.zeros((TOKENS, EXPERTS), jnp.int32).at[row_ids[:, None], expert_ids].add(1)
    blocked = onehot.reshape(TOKENS // TOK_DEV, TOK_DEV, EXPERTS)
    before = (jnp.cumsum(blocked, axis=1) - blocked).reshape(TOKENS, EXPERTS)
    slot_index = jnp.take_along_axis(before, expert_ids, axis=1).astype(jnp.int32)
    position = ((row_ids // TOK_DEV)[:, None] * CAP + slot_index).astype(jnp.int32)
    pair_index = jnp.arange(pair_count, dtype=jnp.int32).reshape(TOKENS, TOP)
    slot_table = jnp.full((EXPERTS, DEVICES * CAP), pair_count, jnp.int32).at[expert_ids, position].set(pair_index)
    padded_tokens = jnp.concatenate([tokens, jnp.zeros((1, D), jnp.bfloat16)], axis=0)
    padded_cotangent = jnp.concatenate([cotangent, jnp.zeros((1, D), jnp.bfloat16)], axis=0)
    padded_gates = jnp.concatenate([gate_weights.reshape(-1), jnp.zeros((1,), jnp.bfloat16)], axis=0)

    def visit(totals, packed):
        slot_rows, weight = packed
        token_rows = slot_rows // TOP
        inputs = padded_tokens[token_rows]
        parts = expert_grads(inputs, padded_cotangent[token_rows],
                             padded_gates[slot_rows].astype(jnp.float32), weight)
        w_grads = weight_terms(inputs, parts[2], parts[3], parts[5], parts[4]).astype(jnp.bfloat16)
        input_b = lax.optimization_barrier(parts[0].astype(jnp.bfloat16))
        gate_b = lax.optimization_barrier(parts[1].astype(jnp.bfloat16))
        input_total = totals[0].at[token_rows].add(input_b.astype(jnp.float32))
        gate_total = totals[1].at[slot_rows].set(gate_b.astype(jnp.float32))
        return (input_total, gate_total), w_grads

    init = (jnp.zeros((TOKENS + 1, D), jnp.float32), jnp.zeros((pair_count + 1,), jnp.float32))
    totals, grad_experts = lax.scan(visit, init, (slot_table, expert_weights))
    shared = expert_grads(tokens, cotangent, jnp.ones((TOKENS,), jnp.float32), shared_weights)
    grad_shared = weight_terms(tokens, shared[2], shared[3], shared[5], shared[4])
    grad_tokens = (totals[0][:TOKENS] + shared[0]).astype(jnp.bfloat16)
    grad_gates = totals[1][:pair_count].reshape(TOKENS, TOP).astype(jnp.bfloat16)
    return grad_tokens, grad_gates, grad_experts, grad_shared
```

```python
import functools

import jax
import jax.numpy as jnp
from jax import lax
from jax.experimental import pallas as pl
from jax.experimental.pallas import tpu as pltpu
from jax.sharding import PartitionSpec as P

MESH = pl.DeviceIdType.MESH
BF = jnp.bfloat16
F32 = jnp.float32
NY, NC, NX, NZ = 4, 2, 4, 8
NPL = NY * NC * NX
CAP = 6
CH = 16
NCH = NZ * CAP // CH
SEQ = (0, 1, 7, 2, 6, 3, 5, 4)
POS = {j: q for q, j in enumerate(SEQ)}
BLOCKS = tuple((c * CH // CAP, -(-(c + 1) * CH // CAP)) for c in range(NCH))
ORDER = tuple(
    (i * 8 + c * 4 + (i + j) % 4) for j in range(4) for c in range(2) for i in range(4)
)
ORDER = tuple(o for o in ORDER if o)


def coords():
    d = lax.axis_index("dp")
    e = lax.axis_index("expert")
    return d // 2, d % 2, e % 4, e // 4


def plane_peer(o, sign=1):
    y, c, x, z = coords()
    dy, dc, dx = o // 8, (o // 4) % 2, o % 4
    return (
        lax.rem(y + sign * dy + NY, NY) * 2 + lax.rem(c + dc, NC),
        z * NX + lax.rem(x + sign * dx + NX, NX),
    )


def z_peer(j):
    y, c, x, z = coords()
    return (y * 2 + c, lax.rem(z + j + NZ, NZ) * NX + x)


def greet():
    bar = pltpu.get_barrier_semaphore()
    for o in range(1, NPL):
        pl.semaphore_signal(bar, inc=1, device_id=plane_peer(o), device_id_type=MESH)
    for j in range(1, NZ):
        pl.semaphore_signal(bar, inc=1, device_id=z_peer(j), device_id_type=MESH)
    pl.semaphore_wait(bar, NPL - 1 + NZ - 1)


def remote(src, dst, ss, rs, dev):
    return pltpu.make_async_remote_copy(
        src_ref=src, dst_ref=dst, send_sem=ss, recv_sem=rs, device_id=dev, device_id_type=MESH
    )


def pick(rank, chunk, q):
    rows = lax.broadcasted_iota(jnp.int32, (NPL, CH, 128), 1) + (chunk * CH - q * CAP)
    return jnp.broadcast_to(rank[:, None, :], (NPL, CH, 128)) == rows.astype(F32)


def dispatch_kernel(
    x_ref, y_ref, rg_ref, rx, ry, xg, yg, rgo, sx, sy, px, pg, zs, zr, ms, mr, cs, cr
):
    greet()
    metas = []
    for j in range(1, NZ):
        cp = remote(rg_ref.at[j], rgo.at[POS[j]], ms.at[j], mr.at[j], z_peer(j))
        cp.start()
        metas.append(cp)
    rgo[0] = rg_ref[0]

    def ring(j_from, j_to, k, src):
        dst = (xg, yg)[k]
        step = 1 if (j_to - j_from) % NZ == 1 else -1
        i = POS[j_to] * 2 + k
        return remote(src, dst.at[POS[j_to]], zs.at[i], zr.at[i], z_peer(step))

    cps = {}

    def go(j_from, j_to, k):
        src = (x_ref, y_ref)[k] if j_from == 0 else (xg, yg)[k].at[POS[j_from]]
        cps[(j_to, k)] = ring(j_from, j_to, k, src)
        cps[(j_to, k)].start()

    for k in range(2):
        go(0, 1, k)
        go(0, 7, k)
    xg[0] = x_ref[...]
    yg[0] = y_ref[...]
    for m in metas:
        m.wait()

    outs = []

    def pack(chunk):
        q0, q1 = BLOCKS[chunk]
        width = (q1 - q0) * 128
        for q in range(q0, q1):
            rank = rgo[q, 0:NPL, :].astype(F32)
            gate = rgo[q, NPL : 2 * NPL, :].astype(F32)
            hit = pick(rank, chunk, q)
            lanes = slice((q - q0) * 128, (q - q0 + 1) * 128)
            px[:, lanes] = jnp.where(hit, 1.0, 0.0).astype(BF).reshape(NPL * CH, 128)
            gates = jnp.broadcast_to(gate[:, None, :], (NPL, CH, 128))
            pg[:, lanes] = jnp.where(hit, gates, 0.0).astype(BF).reshape(NPL * CH, 128)

        def group(g, carry):
            rows = pl.ds(pl.multiple_of(g * 128, 128), 128)
            for sel, blk, out in ((px, xg, sx), (pg, yg, sy)):
                data = blk[q0:q1].reshape(width, blk.shape[2])
                got = jnp.dot(sel[rows, 0:width], data, preferred_element_type=F32)
                out[chunk, pl.ds(pl.multiple_of(g * 8, 8), 8)] = got.astype(BF).reshape(
                    8, CH, blk.shape[2]
                )
            return carry

        lax.fori_loop(0, NPL // 8, group, 0)
        rx[chunk, 0] = sx[chunk, 0]
        ry[chunk, 0] = sy[chunk, 0]
        for o in ORDER:
            for k, (s, r) in enumerate(((sx, rx), (sy, ry))):
                cp = remote(
                    s.at[chunk, o],
                    r.at[chunk, o],
                    cs.at[k, chunk, o],
                    cr.at[k, chunk, o],
                    plane_peer(o),
                )
                cp.start()
                outs.append(cp)

    def arrived(*keys):
        for key in keys:
            cps[key].wait_recv()

    for k in range(2):
        arrived((1, k))
        go(1, 2, k)
        arrived((7, k))
        go(7, 6, k)
    pack(0)
    for k in range(2):
        arrived((2, k))
        go(2, 3, k)
        arrived((6, k))
        go(6, 5, k)
    arrived((3, 0))
    go(3, 4, 0)
    arrived((5, 1))
    go(5, 4, 1)
    arrived((3, 1), (5, 0))
    pack(1)
    arrived((4, 0), (4, 1))
    pack(2)
    for key in cps:
        cps[key].wait_send()
    for cp in outs:
        cp.wait()


def dispatch(x, y, rg):
    t, d = x.shape
    vm = pl.BlockSpec(memory_space=pltpu.VMEM)
    rows = jax.ShapeDtypeStruct((NCH, NPL, CH, d), BF)
    return pl.pallas_call(
        dispatch_kernel,
        out_shape=(
            rows,
            rows,
            jax.ShapeDtypeStruct((NZ, t, d), BF),
            jax.ShapeDtypeStruct((NZ, t, d), BF),
            jax.ShapeDtypeStruct((NZ, 2 * NPL, t), BF),
        ),
        in_specs=[vm] * 3,
        out_specs=(vm,) * 5,
        scratch_shapes=[
            pltpu.VMEM((NCH, NPL, CH, d), BF),
            pltpu.VMEM((NCH, NPL, CH, d), BF),
            pltpu.VMEM((NPL * CH, 4 * 128), BF),
            pltpu.VMEM((NPL * CH, 4 * 128), BF),
            pltpu.SemaphoreType.DMA((2 * NZ,)),
            pltpu.SemaphoreType.DMA((2 * NZ,)),
            pltpu.SemaphoreType.DMA((NZ,)),
            pltpu.SemaphoreType.DMA((NZ,)),
            pltpu.SemaphoreType.DMA((2, NCH, NPL)),
            pltpu.SemaphoreType.DMA((2, NCH, NPL)),
        ],
        compiler_params=pltpu.CompilerParams(
            collective_id=0, has_side_effects=True, vmem_limit_bytes=60 << 20
        ),
        name="dispatch",
    )(x, y, rg)


def collect_kernel(
    dx_ref, gs_ref, rg_ref, sp_ref, gsh_ref,
    out, dgo, sho, ret, gsr, zsend, zrecv, dsend, sh1, sh2,
    cs, cr, gss, gsrs, zs, zr, ds, dr, s1s, s1r, s2s, s2r, s3s, s3r,
):
    y, c, x, z = coords()
    greet()
    sends = []

    def start(cp):
        cp.start()
        sends.append(cp)
        return cp

    dps = [o for o in range(0, NPL, 4)]
    part1 = []
    for i, o in enumerate(dps):
        if o == 0:
            continue
        dev = plane_peer(o)
        src = gsh_ref.at[:, pl.ds(pl.multiple_of(dev[0] * 128, 128), 128)]
        part1.append(start(remote(src, sh1.at[i], s1s.at[i], s1r.at[i], dev)))
    gates = []
    for o in ORDER:
        gates.append(
            start(remote(gs_ref.at[o], gsr.at[o], gss.at[o], gsrs.at[o], plane_peer(o, -1)))
        )
    gsr[0] = gs_ref[0]
    rows = []
    for chunk in range(NCH):
        got = []
        for o in ORDER:
            got.append(
                start(
                    remote(
                        dx_ref.at[chunk, o],
                        ret.at[chunk, o],
                        cs.at[chunk, o],
                        cr.at[chunk, o],
                        plane_peer(o, -1),
                    )
                )
            )
        ret[chunk, 0] = dx_ref[chunk, 0]
        rows.append(got)

    for cp in part1:
        cp.wait_recv()
    mine = pl.ds(pl.multiple_of((y * 2 + c) * 128, 128), 128)
    total = gsh_ref[:, mine]
    for i in range(1, len(dps)):
        total = total + sh1[i]
    sh2[0] = total
    part2 = []
    for o in (1, 3, 2):
        part2.append(start(remote(sh2.at[0], sh2.at[o], s2s.at[o], s2r.at[o], plane_peer(o))))
    for cp in part2:
        cp.wait_recv()
    sho[z] = sh2[0] + sh2[1] + sh2[2] + sh2[3]
    part3 = []
    for j in (1, 7, 2, 6, 3, 5, 4):
        part3.append(start(remote(sho.at[z], sho.at[z], s3s.at[j], s3r.at[j], z_peer(j))))

    for cp in gates:
        cp.wait_recv()
    lane = lax.broadcasted_iota(jnp.int32, (NPL, CH, 128), 2)
    row = lax.broadcasted_iota(jnp.int32, (NPL, CH, 128), 1)
    zgot = []
    done = 0
    for chunk in range(NCH):
        for cp in rows[chunk]:
            cp.wait_recv()
        q0, q1 = BLOCKS[chunk]
        spread = jnp.broadcast_to(gsr[:, 0, :][:, None, :], (NPL, CH, 128))
        value = jnp.sum(
            jnp.where(lane == row + chunk * CH, spread, 0.0), axis=2, keepdims=True
        )
        for q in range(q0, q1):
            rank = rg_ref[q, 0:NPL, :].astype(F32)
            hit = pick(rank, chunk, q)
            sel = jnp.where(hit, 1.0, 0.0).astype(BF).reshape(NPL * CH, 128)
            dterm = jnp.sum(jnp.where(hit, value, 0.0), axis=1)
            part = lax.dot_general(
                sel,
                ret[chunk].reshape(NPL * CH, ret.shape[3]),
                (((0,), (0,)), ((), ())),
                preferred_element_type=F32,
            )
            if q * CAP < chunk * CH:
                sp_ref[q] = sp_ref[q] + part
                dsend[q] = dsend[q] + dterm
            else:
                sp_ref[q] = sp_ref[q] + part
                dsend[q] = dterm
            if (q + 1) * CAP <= (chunk + 1) * CH and q > 0:
                j = SEQ[q]
                zsend[q] = sp_ref[q].astype(BF)
                zgot.append(start(remote(zsend.at[q], zrecv.at[q], zs.at[q], zr.at[q], z_peer(-j))))
                zgot.append(start(remote(dsend.at[q], dgo.at[j], ds.at[q], dr.at[q], z_peer(-j))))
    dgo[0] = dsend[0]
    for cp in zgot:
        cp.wait_recv()
    acc = sp_ref[0]
    for q in range(1, NZ):
        acc = acc + zrecv[q].astype(F32)
    out[...] = acc.astype(BF)
    for cp in part3:
        cp.wait_recv()
    for cp in sends:
        cp.wait_send()


def collect(dx, gs, rg, sp, gsh):
    d = dx.shape[-1]
    t = rg.shape[-1]
    n3 = gsh.shape[0]
    vm = pl.BlockSpec(memory_space=pltpu.VMEM)
    dma = pltpu.SemaphoreType.DMA

    def body(dx_ref, gs_ref, rg_ref, sp_ref, gsh_ref, out, dgo, sho, acc, *rest):
        acc[...] = sp_ref[...]
        collect_kernel(dx_ref, gs_ref, rg_ref, acc, gsh_ref, out, dgo, sho, *rest)

    return pl.pallas_call(
        body,
        out_shape=(
            jax.ShapeDtypeStruct((t, d), BF),
            jax.ShapeDtypeStruct((NZ, NPL, t), F32),
            jax.ShapeDtypeStruct((NZ, n3, 128), F32),
        ),
        in_specs=[vm] * 5,
        out_specs=(vm,) * 3,
        scratch_shapes=[
            pltpu.VMEM((NZ, t, d), F32),
            pltpu.VMEM((NCH, NPL, CH, d), BF),
            pltpu.VMEM((NPL, 1, 128), F32),
            pltpu.VMEM((NZ, t, d), BF),
            pltpu.VMEM((NZ, t, d), BF),
            pltpu.VMEM((NZ, NPL, t), F32),
            pltpu.VMEM((8, n3, 128), F32),
            pltpu.VMEM((4, n3, 128), F32),
            dma((NCH, NPL)), dma((NCH, NPL)),
            dma((NPL,)), dma((NPL,)),
            dma((NZ,)), dma((NZ,)), dma((NZ,)), dma((NZ,)),
            dma((8,)), dma((8,)), dma((4,)), dma((4,)), dma((NZ,)), dma((NZ,)),
        ],
        compiler_params=pltpu.CompilerParams(
            collective_id=1, has_side_effects=True, vmem_limit_bytes=60 << 20
        ),
        name="collect",
    )(dx, gs, rg, sp, gsh)


def silu_parts(pre):
    sigma = jax.nn.sigmoid(pre)
    return (pre * sigma, sigma * (1.0 + pre * (1.0 - sigma)))


def dot(a, b, dims):
    return lax.dot_general(a, b, ((dims[0], dims[1]), ((), ())), preferred_element_type=F32)


def units(x, gy, weight):
    pre_gate = dot(x, weight[0], ((1,), (0,)))
    pre_up = dot(x, weight[1], ((1,), (0,)))
    back = dot(gy, weight[2], ((1,), (0,)))
    activated, slope = silu_parts(pre_gate)
    hidden = activated * pre_up
    gate_grad = jnp.sum(hidden * back, axis=1)
    ggi = (back * pre_up * slope).astype(BF)
    gui = (back * activated).astype(BF)
    return ggi, gui, hidden.astype(BF), gate_grad


def shards(tokens, cotangent, expert_ids, gate_weights, expert_weights, shared_weights):
    t, d = tokens.shape
    y, c, x, z = coords()
    r = jnp.arange(NZ * NPL, dtype=jnp.int32)
    j, o = r // NPL, r % NPL
    dy, dc, dx = o // 8, (o // 4) % 2, o % 4
    owner = (((y + dy) % NY) * 2 + (c + dc) % NC) * (NZ * NX) + ((z + j) % NZ) * NX + (x + dx) % NX
    match = expert_ids.T[:, None, :] == owner[None, :, None]
    named = jnp.any(match, axis=0)
    gate = jnp.sum(jnp.where(match, gate_weights.astype(F32).T[:, None, :], 0.0), axis=0)
    ids = jnp.arange(t, dtype=jnp.int32)
    earlier = (ids[:, None] < ids[None, :]).astype(BF)
    rank = jnp.dot(named.astype(BF), earlier, preferred_element_type=F32)
    rank = jnp.where(named, rank, -100.0)
    rg = jnp.concatenate(
        [rank.astype(BF).reshape(NZ, NPL, t), gate.astype(BF).reshape(NZ, NPL, t)], axis=1
    )
    rx, ry, xg, yg, rgo = dispatch(tokens, cotangent, rg)

    slots = NCH * NPL * CH
    w = expert_weights[0]
    ex, ey = rx.reshape(slots, d), ry.reshape(slots, d)
    ggi, gui, hid, gate_grad = units(ex, ey, w)
    dxr = dot(ggi, w[0], ((1,), (1,))) + dot(gui, w[1], ((1,), (1,)))
    dxr = dxr.astype(BF).reshape(NCH, NPL, CH, d)
    gs = gate_grad.reshape(NCH, NPL, CH).transpose(1, 0, 2).reshape(NPL, 1, NCH * CH)
    gs = jnp.pad(gs, ((0, 0), (0, 0), (0, 128 - NCH * CH)))

    f = shared_weights.shape[2] // NZ
    sw = lax.dynamic_slice_in_dim(shared_weights, z * f, f, 2)
    sx, sy = xg.reshape(NZ * t, d), yg.reshape(NZ * t, d)
    sggi, sgui, shid, _ = units(sx, sy, sw)
    sp = dot(sggi, sw[0], ((1,), (1,))) + dot(sgui, sw[1], ((1,), (1,)))
    gsh = jnp.concatenate(
        [
            dot(sggi, sx, ((0,), (0,))),
            dot(sgui, sx, ((0,), (0,))),
            dot(shid, sy, ((0,), (0,))),
        ],
        axis=0,
    )
    grad_tokens, dg, sh = collect(dxr, gs, rgo, sp.reshape(NZ, t, d), gsh)

    grad_experts = jnp.stack(
        [
            dot(ex, ggi, ((0,), (0,))),
            dot(ex, gui, ((0,), (0,))),
            dot(ey, hid, ((0,), (0,))),
        ],
        axis=0,
    ).astype(BF)[None]
    dgr = dg.reshape(NZ * NPL, t)
    picked = jnp.sum(jnp.where(match, dgr[None], 0.0), axis=1)
    grad_gates = (picked.T / gate_weights.astype(F32)).astype(BF)
    grad_shared = sh.reshape(NZ, 3, f, 128).transpose(1, 3, 0, 2).reshape(3, 128, NZ * f)
    return (grad_tokens, grad_gates, grad_experts, grad_shared)


def solution(mesh):
    rows = P(("dp", "expert"), None)
    return jax.shard_map(
        shards,
        mesh=mesh,
        in_specs=(rows, rows, rows, rows, P(("dp", "expert"), None, None, None), P()),
        out_specs=(rows, rows, P(("dp", "expert"), None, None, None), P(None, "dp", None)),
        check_vma=False,
    )
```

```python
import functools

import jax
import jax.numpy as jnp
from jax import lax
from jax.experimental import pallas as pl
from jax.experimental.pallas import tpu as pltpu
from jax.sharding import PartitionSpec as P

MESH = pl.DeviceIdType.MESH
BF = jnp.bfloat16
F32 = jnp.float32
NY, NC, NX, NZ = 4, 2, 4, 8
NPL = NY * NC * NX
CAP = 6
CH = 16
NCH = NZ * CAP // CH
SEQ = (0, 1, 7, 2, 6, 3, 5, 4)
POS = {j: q for q, j in enumerate(SEQ)}
BLOCKS = tuple((c * CH // CAP, -(-(c + 1) * CH // CAP)) for c in range(NCH))
ORDER = tuple(
    (i * 8 + c * 4 + (i + j) % 4) for j in range(4) for c in range(2) for i in range(4)
)
ORDER = tuple(o for o in ORDER if o)


def coords():
    d = lax.axis_index("dp")
    e = lax.axis_index("expert")
    return d // 2, d % 2, e % 4, e // 4


def plane_peer(o, sign=1):
    y, c, x, z = coords()
    dy, dc, dx = o // 8, (o // 4) % 2, o % 4
    return (
        lax.rem(y + sign * dy + NY, NY) * 2 + lax.rem(c + dc, NC),
        z * NX + lax.rem(x + sign * dx + NX, NX),
    )


def z_peer(j):
    y, c, x, z = coords()
    return (y * 2 + c, lax.rem(z + j + NZ, NZ) * NX + x)


def greet():
    bar = pltpu.get_barrier_semaphore()
    for o in range(1, NPL):
        pl.semaphore_signal(bar, inc=1, device_id=plane_peer(o), device_id_type=MESH)
    for j in range(1, NZ):
        pl.semaphore_signal(bar, inc=1, device_id=z_peer(j), device_id_type=MESH)
    pl.semaphore_wait(bar, NPL - 1 + NZ - 1)


def remote(src, dst, ss, rs, dev):
    return pltpu.make_async_remote_copy(
        src_ref=src, dst_ref=dst, send_sem=ss, recv_sem=rs, device_id=dev, device_id_type=MESH
    )


def pick(rank, chunk, q):
    rows = lax.broadcasted_iota(jnp.int32, (NPL, CH, 128), 1) + (chunk * CH - q * CAP)
    return jnp.broadcast_to(rank[:, None, :], (NPL, CH, 128)) == rows.astype(F32)


def dot(a, b, ca, cb):
    return lax.dot_general(a, b, (((ca,), (cb,)), ((), ())), preferred_element_type=F32)


def units(pre_gate, pre_up, back):
    sigma = jax.nn.sigmoid(pre_gate)
    activated = pre_gate * sigma
    slope = sigma * (1.0 + pre_gate * (1.0 - sigma))
    hidden = activated * pre_up
    ggi = (back * pre_up * slope).astype(BF)
    gui = (back * activated).astype(BF)
    return ggi, gui, hidden


def layer_kernel(
    x_ref, y_ref, rg_ref, w_hbm, sw_ref,
    out, dgo, ge, gsho,
    w, rx, ry, xg, yg, rgo, sx, sy, px, pg,
    ggi, gui, hid, dxr, ret, gs, gsr, acc, gsh, gshb, sh1, sh2, sh3, zout, zin, dsend,
    wsem, zs, zr, ms, mr, cs, cr, bs, br, gss, grs, us, ur, ds, dr, s1s, s1r, s2s, s2r, s3s, s3r,
):
    y, c, x, z = coords()
    d = x_ref.shape[1]
    f = w.shape[2]
    sends = []

    def start(cp):
        cp.start()
        sends.append(cp)
        return cp

    load = pltpu.make_async_copy(w_hbm.at[0], w, wsem)
    load.start()
    greet()

    metas = []
    for j in range(1, NZ):
        metas.append(
            start(remote(rg_ref.at[j], rgo.at[POS[j]], ms.at[j], mr.at[j], z_peer(j)))
        )
    rgo[0] = rg_ref[0]

    cps = {}

    def go(j_from, j_to, k):
        src = (x_ref, y_ref)[k] if j_from == 0 else (xg, yg)[k].at[POS[j_from]]
        step = 1 if (j_to - j_from) % NZ == 1 else -1
        i = POS[j_to] * 2 + k
        dst = (xg, yg)[k].at[POS[j_to]]
        cps[(j_to, k)] = start(remote(src, dst, zs.at[i], zr.at[i], z_peer(step)))

    def arrived(*keys):
        for key in keys:
            cps[key].wait_recv()

    for k in range(2):
        go(0, 1, k)
        go(0, 7, k)
    xg[0] = x_ref[...]
    yg[0] = y_ref[...]
    for m in metas:
        m.wait_recv()

    rows_in = {}

    def pack(chunk):
        q0, q1 = BLOCKS[chunk]
        width = (q1 - q0) * 128
        for q in range(q0, q1):
            rank = rgo[q, 0:NPL, :].astype(F32)
            gate = rgo[q, NPL : 2 * NPL, :].astype(F32)
            hit = pick(rank, chunk, q)
            lanes = slice((q - q0) * 128, (q - q0 + 1) * 128)
            px[:, lanes] = jnp.where(hit, 1.0, 0.0).astype(BF).reshape(NPL * CH, 128)
            gates = jnp.broadcast_to(gate[:, None, :], (NPL, CH, 128))
            pg[:, lanes] = jnp.where(hit, gates, 0.0).astype(BF).reshape(NPL * CH, 128)

        def group(g, carry):
            rows = pl.ds(pl.multiple_of(g * 128, 128), 128)
            for sel, blk, dst in ((px, xg, sx), (pg, yg, sy)):
                data = blk[q0:q1].reshape(width, d)
                got = dot(sel[rows, 0:width], data, 1, 0)
                dst[chunk, pl.ds(pl.multiple_of(g * 8, 8), 8)] = got.astype(BF).reshape(8, CH, d)
            return carry

        lax.fori_loop(0, NPL // 8, group, 0)
        rx[chunk, 0] = sx[chunk, 0]
        ry[chunk, 0] = sy[chunk, 0]
        got = []
        for o in ORDER:
            for k, (s, r) in enumerate(((sx, rx), (sy, ry))):
                sem = (k, chunk, o)
                got.append(
                    start(
                        remote(
                            s.at[chunk, o], r.at[chunk, o], cs.at[sem], cr.at[sem], plane_peer(o)
                        )
                    )
                )
        rows_in[chunk] = got

    for k in range(2):
        arrived((1, k))
        go(1, 2, k)
        arrived((7, k))
        go(7, 6, k)
    pack(0)
    for k in range(2):
        arrived((2, k))
        go(2, 3, k)
        arrived((6, k))
        go(6, 5, k)
    arrived((3, 0))
    go(3, 4, 0)
    arrived((5, 1))
    go(5, 4, 1)
    arrived((3, 1), (5, 0))
    pack(1)
    arrived((4, 0), (4, 1))
    pack(2)

    gsh[...] = jnp.zeros_like(gsh)

    def shared(g, carry):
        two = pl.ds(pl.multiple_of(g * 2, 2), 2)
        bx = xg[two].reshape(256, d)
        by = yg[two].reshape(256, d)
        a, b, hidden = units(
            dot(bx, sw_ref[0], 1, 0), dot(bx, sw_ref[1], 1, 0), dot(by, sw_ref[2], 1, 0)
        )
        n = sw_ref.shape[2]
        acc[two] = (dot(a, sw_ref[0], 1, 1) + dot(b, sw_ref[1], 1, 1)).reshape(2, 128, d)
        gsh[0:n, :] += dot(a, bx, 0, 0)
        gsh[n : 2 * n, :] += dot(b, bx, 0, 0)
        gsh[2 * n : 3 * n, :] += dot(hidden.astype(BF), by, 0, 0)
        return carry

    lax.fori_loop(0, NZ // 2, shared, 0)
    gshb[...] = gsh[...].astype(BF)
    part1 = []
    for i in range(1, 8):
        dev = plane_peer(i * 4)
        src = gshb.at[:, pl.ds(pl.multiple_of(dev[0] * 128, 128), 128)]
        part1.append(start(remote(src, sh1.at[i], s1s.at[i], s1r.at[i], dev)))
    load.wait()

    lane3 = lax.broadcasted_iota(jnp.int32, (16, CH, 128), 2)
    row3 = lax.broadcasted_iota(jnp.int32, (16, CH, 128), 1)

    def expert(chunk):
        for cp in rows_in[chunk]:
            cp.wait_recv()

        def group(g, carry):
            os = pl.ds(pl.multiple_of(g * 16, 16), 16)
            rs = pl.ds(pl.multiple_of(chunk * 512 + g * 256, 256), 256)
            bx = rx[chunk, os].reshape(256, d)
            by = ry[chunk, os].reshape(256, d)
            back = dot(by, w[2], 1, 0)
            a, b, hidden = units(dot(bx, w[0], 1, 0), dot(bx, w[1], 1, 0), back)
            ggi[rs, :] = a
            gui[rs, :] = b
            hid[rs, :] = hidden.astype(BF)
            gg = jnp.sum(hidden * back, axis=1, keepdims=True).reshape(16, CH, 1)
            term = jnp.where(lane3 == row3 + chunk * CH, gg, 0.0)
            term = jnp.sum(term, axis=1, keepdims=True)
            if chunk == 0:
                gs[os] = term
            else:
                gs[os] = gs[os] + term
            grads = dot(a, w[0], 1, 1) + dot(b, w[1], 1, 1)
            dxr[chunk, os] = grads.astype(BF).reshape(16, CH, d)
            return carry

        lax.fori_loop(0, 2, group, 0)

    rows_back = {}

    def give_back(chunk):
        got = []
        for o in ORDER:
            sem = (chunk, o)
            got.append(
                start(
                    remote(
                        dxr.at[chunk, o], ret.at[chunk, o], bs.at[sem], br.at[sem],
                        plane_peer(o, -1),
                    )
                )
            )
        ret[chunk, 0] = dxr[chunk, 0]
        rows_back[chunk] = got

    expert(0)
    expert(1)
    give_back(1)
    expert(2)
    give_back(2)
    give_back(0)
    gates = []
    for o in ORDER:
        gates.append(start(remote(gs.at[o], gsr.at[o], gss.at[o], grs.at[o], plane_peer(o, -1))))
    gsr[0] = gs[0]

    for cp in part1:
        cp.wait_recv()
    mine = pl.ds(pl.multiple_of((y * 2 + c) * 128, 128), 128)
    total = gsh[:, mine]
    for i in range(1, 8):
        total = total + sh1[i].astype(F32)
    sh2[0] = total.astype(BF)
    part2 = []
    for o in (1, 3, 2):
        part2.append(start(remote(sh2.at[0], sh2.at[o], s2s.at[o], s2r.at[o], plane_peer(o))))

    def wgrad(g, carry):
        cols = pl.ds(pl.multiple_of(g * 256, 256), 256)
        bx = rx[:, :, :, cols].reshape(NCH * NPL * CH, 256)
        ge[0, cols, :] = dot(bx, ggi[...], 0, 0).astype(BF)
        ge[1, cols, :] = dot(bx, gui[...], 0, 0).astype(BF)
        by = ry[:, :, :, cols].reshape(NCH * NPL * CH, 256)
        ge[2, cols, :] = dot(by, hid[...], 0, 0).astype(BF)
        return carry

    lax.fori_loop(0, d // 256, wgrad, 0)

    for cp in part2:
        cp.wait_recv()
    total = sh2[0].astype(F32)
    for o in range(1, 4):
        total = total + sh2[o].astype(F32)
    sh3[z] = total.astype(BF)
    part3 = []
    for j in (1, 7, 2, 6, 3, 5, 4):
        part3.append(start(remote(sh3.at[z], sh3.at[z], s3s.at[j], s3r.at[j], z_peer(j))))

    lane = lax.broadcasted_iota(jnp.int32, (NPL, CH, 128), 2)
    row = lax.broadcasted_iota(jnp.int32, (NPL, CH, 128), 1)
    for cp in gates:
        cp.wait_recv()
    seen = set()
    left = {q: sum(b0 <= q < b1 for b0, b1 in BLOCKS) for q in range(NZ)}
    dgot = []

    def combine(chunk):
        for cp in rows_back[chunk]:
            cp.wait_recv()
        spread = jnp.broadcast_to(gsr[...], (NPL, CH, 128))
        value = jnp.sum(jnp.where(lane == row + chunk * CH, spread, 0.0), axis=2, keepdims=True)
        for q in reversed(range(*BLOCKS[chunk])):
            hit = pick(rgo[q, 0:NPL, :].astype(F32), chunk, q)
            sel = jnp.where(hit, 1.0, 0.0).astype(BF).reshape(NPL * CH, 128)
            acc[q] = acc[q] + dot(sel, ret[chunk].reshape(NPL * CH, d), 0, 0)
            dterm = jnp.sum(jnp.where(hit, value, 0.0), axis=1)
            dsend[q] = dsend[q] + dterm if q in seen else dterm
            seen.add(q)
            left[q] -= 1
            if not left[q] and q:
                j = SEQ[q]
                dgot.append(start(remote(dsend.at[q], dgo.at[j], ds.at[q], dr.at[q], z_peer(-j))))

    ring = {}

    def pass_on(j):
        lo = slice(0, d // 2)
        hi = slice(d // 2, d)
        q = POS[j]
        if j == 4:
            zout[4] = acc[q].astype(BF)
            ring[3] = start(
                remote(zout.at[4, :, lo], zin.at[3, :, lo], us.at[3], ur.at[3], z_peer(-1))
            )
            ring[5] = start(
                remote(zout.at[4, :, hi], zin.at[5, :, hi], us.at[5], ur.at[5], z_peer(1))
            )
            return
        ring[j].wait_recv()
        part = {3: lo, 5: hi}.get(j, slice(0, d))
        acc[q, :, part] = acc[q, :, part] + zin[j, :, part].astype(F32)
        zout[j] = acc[q].astype(BF)
        if j < 4:
            to, dev = j - 1, z_peer(-1)
        else:
            to, dev = (j + 1) % NZ or 4, z_peer(1)
        ring[to] = start(remote(zout.at[j], zin.at[to], us.at[to], ur.at[to], dev))

    combine(1)
    combine(2)
    for j in (4, 5, 3, 6, 2):
        pass_on(j)
    combine(0)
    for j in (7, 1):
        pass_on(j)
    dgo[0] = dsend[0]
    for cp in part3:
        cp.wait_recv()
    n = sw_ref.shape[2]
    for k in range(3):
        for m in range(NZ // 2):
            pair = [sh3[2 * m + i, k * n : (k + 1) * n, :].astype(F32) for i in range(2)]
            gsho[k, :, m * 2 * n : (m + 1) * 2 * n] = jnp.concatenate(pair, axis=0).T
    for cp in dgot:
        cp.wait_recv()
    ring[4].wait_recv()
    ring[0].wait_recv()
    out[...] = (acc[0] + zin[0].astype(F32) + zin[4].astype(F32)).astype(BF)
    for cp in sends:
        cp.wait_send()


def layer(xs, ys, rg, weights, sw):
    t, d = xs.shape
    f = weights.shape[3]
    n = sw.shape[2]
    slots = NCH * NPL * CH
    vm = pl.BlockSpec(memory_space=pltpu.VMEM)
    hbm = pl.BlockSpec(memory_space=pl.ANY)
    dma = pltpu.SemaphoreType.DMA
    v = pltpu.VMEM
    return pl.pallas_call(
        layer_kernel,
        out_shape=(
            jax.ShapeDtypeStruct((t, d), BF),
            jax.ShapeDtypeStruct((NZ, NPL, t), F32),
            jax.ShapeDtypeStruct((3, d, f), BF),
            jax.ShapeDtypeStruct((3, 128, NZ * n), F32),
        ),
        in_specs=[vm, vm, vm, hbm, vm],
        out_specs=(vm,) * 4,
        scratch_shapes=[
            v((3, d, f), BF),
            v((NCH, NPL, CH, d), BF), v((NCH, NPL, CH, d), BF),
            v((NZ, t, d), BF), v((NZ, t, d), BF), v((NZ, 2 * NPL, t), BF),
            v((NCH, NPL, CH, d), BF), v((NCH, NPL, CH, d), BF),
            v((NPL * CH, 512), BF), v((NPL * CH, 512), BF),
            v((slots, f), BF), v((slots, f), BF), v((slots, f), BF),
            v((NCH, NPL, CH, d), BF), v((NCH, NPL, CH, d), BF),
            v((NPL, 1, 128), F32), v((NPL, 1, 128), F32),
            v((NZ, t, d), F32),
            v((3 * n, d), F32), v((3 * n, d), BF),
            v((8, 3 * n, 128), BF), v((4, 3 * n, 128), BF), v((NZ, 3 * n, 128), BF),
            v((NZ, t, d), BF), v((NZ, t, d), BF),
            v((NZ, NPL, t), F32),
            dma,
            dma((2 * NZ,)), dma((2 * NZ,)), dma((NZ,)), dma((NZ,)),
            dma((2, NCH, NPL)), dma((2, NCH, NPL)), dma((NCH, NPL)), dma((NCH, NPL)),
            dma((NPL,)), dma((NPL,)), dma((NZ,)), dma((NZ,)), dma((NZ,)), dma((NZ,)),
            dma((8,)), dma((8,)), dma((4,)), dma((4,)), dma((NZ,)), dma((NZ,)),
        ],
        compiler_params=pltpu.CompilerParams(
            collective_id=0, has_side_effects=True, vmem_limit_bytes=61 << 20
        ),
        name="layer",
    )(xs, ys, rg, weights, sw)


def shards(tokens, cotangent, expert_ids, gate_weights, expert_weights, shared_weights):
    t, d = tokens.shape
    y, c, x, z = coords()
    r = jnp.arange(NZ * NPL, dtype=jnp.int32)
    j, o = r // NPL, r % NPL
    dy, dc, dx = o // 8, (o // 4) % 2, o % 4
    owner = (((y + dy) % NY) * 2 + (c + dc) % NC) * (NZ * NX) + ((z + j) % NZ) * NX + (x + dx) % NX
    match = expert_ids.T[:, None, :] == owner[None, :, None]
    named = jnp.any(match, axis=0)
    gate = jnp.sum(jnp.where(match, gate_weights.astype(F32).T[:, None, :], 0.0), axis=0)
    ids = jnp.arange(t, dtype=jnp.int32)
    earlier = (ids[:, None] < ids[None, :]).astype(BF)
    rank = jnp.dot(named.astype(BF), earlier, preferred_element_type=F32)
    rank = jnp.where(named, rank, -100.0)
    rg = jnp.concatenate(
        [rank.astype(BF).reshape(NZ, NPL, t), gate.astype(BF).reshape(NZ, NPL, t)], axis=1
    )
    f = shared_weights.shape[2] // NZ
    sw = lax.dynamic_slice_in_dim(shared_weights, z * f, f, 2)
    grad_tokens, dg, ge, grad_shared = layer(tokens, cotangent, rg, expert_weights, sw)
    dgr = dg.reshape(NZ * NPL, t)
    picked = jnp.sum(jnp.where(match, dgr[None], 0.0), axis=1)
    grad_gates = (picked.T / gate_weights.astype(F32)).astype(BF)
    return (grad_tokens, grad_gates, ge[None], grad_shared)


def solution(mesh):
    rows = P(("dp", "expert"), None)
    return jax.shard_map(
        shards,
        mesh=mesh,
        in_specs=(rows, rows, rows, rows, P(("dp", "expert"), None, None, None), P()),
        out_specs=(rows, rows, P(("dp", "expert"), None, None, None), P(None, "dp", None)),
        check_vma=False,
    )
```

```python
import jax
import jax.numpy as jnp
from jax import lax
from jax.experimental import pallas as pl
from jax.experimental.pallas import tpu as pltpu
from jax.sharding import PartitionSpec as P

MESH = pl.DeviceIdType.MESH
BF = jnp.bfloat16
F32 = jnp.float32
NY, NC, NX, NZ = 4, 2, 4, 8
NPL = NY * NC * NX
CAP = 6
CH = 16
NCH = NZ * CAP // CH
SEQ = (0, 1, 7, 2, 6, 3, 5, 4)
POS = {j: q for q, j in enumerate(SEQ)}
BLOCKS = tuple((c * CH // CAP, -(-(c + 1) * CH // CAP)) for c in range(NCH))
ORDER = tuple(
    (i * 8 + c * 4 + (i + j) % 4) for j in range(4) for c in range(2) for i in range(4)
)
ORDER = tuple(o for o in ORDER if o)


def coords():
    d = lax.axis_index("dp")
    e = lax.axis_index("expert")
    return d // 2, d % 2, e % 4, e // 4


def plane_peer(o, sign=1):
    y, c, x, z = coords()
    dy, dc, dx = o // 8, (o // 4) % 2, o % 4
    return (
        lax.rem(y + sign * dy + NY, NY) * 2 + lax.rem(c + dc, NC),
        z * NX + lax.rem(x + sign * dx + NX, NX),
    )


def z_peer(j):
    y, c, x, z = coords()
    return (y * 2 + c, lax.rem(z + j + NZ, NZ) * NX + x)


def owners(j):
    y, c, x, z = coords()
    o = lax.broadcasted_iota(jnp.int32, (NPL, 128), 0)
    dp = lax.rem(y + (o >> 3), NY) * 2 + lax.rem(c + ((o >> 2) & 1), NC)
    return dp * (NZ * NX) + lax.rem(z + j, NZ) * NX + lax.rem(x + (o & 3), NX)


def greet():
    bar = pltpu.get_barrier_semaphore()
    for o in range(1, NPL):
        pl.semaphore_signal(bar, inc=1, device_id=plane_peer(o), device_id_type=MESH)
    for j in range(1, NZ):
        pl.semaphore_signal(bar, inc=1, device_id=z_peer(j), device_id_type=MESH)


def greeted():
    pl.semaphore_wait(pltpu.get_barrier_semaphore(), NPL - 1 + NZ - 1)


def remote(src, dst, ss, rs, dev):
    return pltpu.make_async_remote_copy(
        src_ref=src, dst_ref=dst, send_sem=ss, recv_sem=rs, device_id=dev, device_id_type=MESH
    )


def pick(rank, chunk, q):
    rows = lax.broadcasted_iota(jnp.int32, (NPL, CH, 128), 1) + (chunk * CH - q * CAP)
    return jnp.broadcast_to(rank[:, None, :], (NPL, CH, 128)) == rows.astype(F32)


def dot(a, b, ca, cb):
    return lax.dot_general(a, b, (((ca,), (cb,)), ((), ())), preferred_element_type=F32)


def units(pre_gate, pre_up, back):
    sigma = jax.nn.sigmoid(pre_gate)
    activated = pre_gate * sigma
    slope = sigma * (1.0 + pre_gate * (1.0 - sigma))
    hidden = activated * pre_up
    ggi = (back * pre_up * slope).astype(BF)
    gui = (back * activated).astype(BF)
    return ggi, gui, hidden


def layer_kernel(
    x_hbm, y_hbm, ids_ref, gw_ref, w_hbm, sw_hbm,
    out, ggo, ge_hbm, gs_hbm,
    w, swb, sw_ref, ge, gsho, rg_ref, dgo, rx, ry, xg, yg, rgo, sx, sy, px, pg,
    ggi, gui, hid, dxr, ret, gs, gsr, acc, gsh, gshb, sh1, sh2, sh3, zout, zin, dsend,
    wsem, xsem, ysem, ssem, gsem, fsem, zs, zr, ms, mr, cs, cr, bs, br, gss, grs, us, ur, ds, dr, s1s, s1r, s2s, s2r, s3s, s3r,
):
    y, c, x, z = coords()
    d = x_hbm.shape[1]
    sends = []

    def start(cp):
        cp.start()
        sends.append(cp)
        return cp

    greet()
    own = (
        pltpu.make_async_copy(x_hbm, xg.at[0], xsem),
        pltpu.make_async_copy(y_hbm, yg.at[0], ysem),
    )
    load = pltpu.make_async_copy(w_hbm.at[0], w, wsem)
    halves = pl.ds(pl.multiple_of((z // 2) * 128, 128), 128)
    loads = pltpu.make_async_copy(sw_hbm.at[:, :, halves], swb, ssem)
    own[0].start()
    own[1].start()
    loads.start()
    load.start()
    older = lax.broadcasted_iota(jnp.int32, (128, 128), 0)
    earlier = (older < lax.broadcasted_iota(jnp.int32, (128, 128), 1)).astype(F32).astype(BF)
    for j in range(NZ):
        who = owners(j)
        named = jnp.zeros((NPL, 128), F32)
        gate = jnp.zeros((NPL, 128), F32)
        for k in range(ids_ref.shape[0]):
            hit = ids_ref[k : k + 1, :] == who
            named = jnp.where(hit, 1.0, named)
            gate = jnp.where(hit, gw_ref[k : k + 1, :].astype(F32), gate)
        rank = dot(named.astype(BF), earlier, 1, 0)
        rg_ref[j, 0:NPL, :] = jnp.where(named > 0.5, rank, -100.0).astype(BF)
        rg_ref[j, NPL : 2 * NPL, :] = gate.astype(BF)
    own[0].wait()
    own[1].wait()
    greeted()

    cps = {}

    def go(j_from, j_to, k):
        src = (xg, yg)[k].at[POS[j_from]]
        step = 1 if (j_to - j_from) % NZ == 1 else -1
        i = POS[j_to] * 2 + k
        dst = (xg, yg)[k].at[POS[j_to]]
        cps[(j_to, k)] = start(remote(src, dst, zs.at[i], zr.at[i], z_peer(step)))

    def arrived(*keys):
        for key in keys:
            cps[key].wait_recv()

    metas = []
    for j in range(1, NZ):
        metas.append(
            start(remote(rg_ref.at[j], rgo.at[POS[j]], ms.at[j], mr.at[j], z_peer(j)))
        )
    for k in range(2):
        go(0, 1, k)
        go(0, 7, k)
    rgo[0] = rg_ref[0]

    for m in metas:
        m.wait_recv()

    rows_in = {chunk: [] for chunk in range(NCH)}

    def pack(chunk, k):
        q0, q1 = BLOCKS[chunk]
        width = (q1 - q0) * 128
        sel, blk, snd, rcv = ((px, xg, sx, rx), (pg, yg, sy, ry))[k]
        for q in range(q0, q1):
            hit = pick(rgo[q, 0:NPL, :].astype(F32), chunk, q)
            if k:
                gate = rgo[q, NPL : 2 * NPL, :].astype(F32)
                value = jnp.broadcast_to(gate[:, None, :], (NPL, CH, 128))
            else:
                value = 1.0
            lanes = slice((q - q0) * 128, (q - q0 + 1) * 128)
            sel[:, lanes] = jnp.where(hit, value, 0.0).astype(BF).reshape(NPL * CH, 128)

        def group(g, carry):
            rows = pl.ds(pl.multiple_of(g * 256, 256), 256)
            got = dot(sel[rows, 0:width], blk[q0:q1].reshape(width, d), 1, 0)
            os = pl.ds(pl.multiple_of(g * 16, 16), 16)
            snd[chunk, os] = got.astype(BF).reshape(16, CH, d)
            return carry

        lax.fori_loop(0, NPL // 16, group, 0)
        rcv[chunk, 0] = snd[chunk, 0]
        for o in ORDER:
            sem = (k, chunk, o)
            rows_in[chunk].append(
                start(
                    remote(
                        snd.at[chunk, o], rcv.at[chunk, o], cs.at[sem], cr.at[sem], plane_peer(o)
                    )
                )
            )

    def forward(j_from, j_to, k):
        arrived((j_from, k))
        go(j_from, j_to, k)

    for k in range(2):
        forward(1, 2, k)
        forward(7, 6, k)
        pack(0, k)
    for k in range(2):
        forward(2, 3, k)
        forward(6, 5, k)
    forward(3, 4, 0)
    arrived((5, 0))
    pack(1, 0)
    forward(5, 4, 1)
    arrived((3, 1))
    pack(1, 1)
    arrived((4, 0))
    pack(2, 0)
    arrived((4, 1))
    pack(2, 1)

    loads.wait()
    n = swb.shape[2] // 2
    sw_ref[...] = jnp.where(lax.rem(z, 2) == 1, swb[:, :, n:], swb[:, :, :n])
    gsh[...] = jnp.zeros_like(gsh)

    def shared(g, carry):
        two = pl.ds(pl.multiple_of(g * 2, 2), 2)
        bx = xg[two].reshape(256, d)
        by = yg[two].reshape(256, d)
        a, b, hidden = units(
            dot(bx, sw_ref[0], 1, 0), dot(bx, sw_ref[1], 1, 0), dot(by, sw_ref[2], 1, 0)
        )
        n = sw_ref.shape[2]
        acc[two] = (dot(a, sw_ref[0], 1, 1) + dot(b, sw_ref[1], 1, 1)).reshape(2, 128, d)
        gsh[0:n, :] += dot(a, bx, 0, 0)
        gsh[n : 2 * n, :] += dot(b, bx, 0, 0)
        gsh[2 * n : 3 * n, :] += dot(hidden.astype(BF), by, 0, 0)
        return carry

    lax.fori_loop(0, NZ // 2, shared, 0)
    gshb[...] = gsh[...].astype(BF)
    part1 = []
    for i in range(1, 8):
        dev = plane_peer(i * 4)
        src = gshb.at[:, pl.ds(pl.multiple_of(dev[0] * 128, 128), 128)]
        part1.append(start(remote(src, sh1.at[i], s1s.at[i], s1r.at[i], dev)))
    load.wait()

    lane3 = lax.broadcasted_iota(jnp.int32, (16, CH, 128), 2)
    row3 = lax.broadcasted_iota(jnp.int32, (16, CH, 128), 1)

    def expert(chunk):
        for cp in rows_in[chunk]:
            cp.wait_recv()

        def group(g, carry):
            os = pl.ds(pl.multiple_of(g * 16, 16), 16)
            rs = pl.ds(pl.multiple_of(chunk * 512 + g * 256, 256), 256)
            bx = rx[chunk, os].reshape(256, d)
            by = ry[chunk, os].reshape(256, d)
            back = dot(by, w[2], 1, 0)
            a, b, hidden = units(dot(bx, w[0], 1, 0), dot(bx, w[1], 1, 0), back)
            ggi[rs, :] = a
            gui[rs, :] = b
            hid[rs, :] = hidden.astype(BF)
            gg = jnp.sum(hidden * back, axis=1, keepdims=True).reshape(16, CH, 1)
            term = jnp.where(lane3 == row3 + chunk * CH, gg, 0.0)
            term = jnp.sum(term, axis=1, keepdims=True)
            if chunk == 0:
                gs[os] = term
            else:
                gs[os] = gs[os] + term
            grads = dot(a, w[0], 1, 1) + dot(b, w[1], 1, 1)
            dxr[chunk, os] = grads.astype(BF).reshape(16, CH, d)
            return carry

        lax.fori_loop(0, 2, group, 0)

    rows_back = {}

    lo = slice(0, d // 2)
    hi = slice(d // 2, d)

    def give_back(chunk, sem, part):
        got = []
        for o in ORDER:
            got.append(
                start(
                    remote(
                        dxr.at[chunk, o, :, part], ret.at[chunk, o, :, part],
                        bs.at[sem, o], br.at[sem, o], plane_peer(o, -1),
                    )
                )
            )
        rows_back[sem] = got

    expert(0)
    expert(1)
    give_back(1, 1, slice(0, d))
    expert(2)
    for cp in part1:
        cp.wait_recv()
    mine = pl.ds(pl.multiple_of((y * 2 + c) * 128, 128), 128)
    total = gsh[:, mine]
    for i in range(1, 8):
        total = total + sh1[i].astype(F32)
    sh2[0] = total.astype(BF)
    part2 = []
    for o in (1, 3, 2):
        part2.append(start(remote(sh2.at[0], sh2.at[o], s2s.at[o], s2r.at[o], plane_peer(o))))
    gates = []
    for o in ORDER:
        gates.append(start(remote(gs.at[o], gsr.at[o], gss.at[o], grs.at[o], plane_peer(o, -1))))
    gsr[0] = gs[0]
    give_back(2, 2, slice(0, d))
    give_back(0, 0, lo)
    give_back(0, NCH, hi)
    for chunk in range(NCH):
        ret[chunk, 0] = dxr[chunk, 0]

    def wgrad(g, carry):
        cols = pl.ds(pl.multiple_of(g * 256, 256), 256)
        bx = rx[:, :, :, cols].reshape(NCH * NPL * CH, 256)
        ge[0, cols, :] = dot(bx, ggi[...], 0, 0).astype(BF)
        ge[1, cols, :] = dot(bx, gui[...], 0, 0).astype(BF)
        by = ry[:, :, :, cols].reshape(NCH * NPL * CH, 256)
        ge[2, cols, :] = dot(by, hid[...], 0, 0).astype(BF)
        return carry

    lax.fori_loop(0, d // 256, wgrad, 0)
    save = pltpu.make_async_copy(ge, ge_hbm, gsem)
    save.start()

    for cp in part2:
        cp.wait_recv()
    total = sh2[0].astype(F32)
    for o in range(1, 4):
        total = total + sh2[o].astype(F32)
    sh3[z] = total.astype(BF)
    part3 = []
    for j in (1, 7, 2, 6, 3, 5, 4):
        part3.append(start(remote(sh3.at[z], sh3.at[z], s3s.at[j], s3r.at[j], z_peer(j))))

    lane = lax.broadcasted_iota(jnp.int32, (NPL, CH, 128), 2)
    row = lax.broadcasted_iota(jnp.int32, (NPL, CH, 128), 1)
    for cp in gates:
        cp.wait_recv()
    seen = set()
    left = {q: sum(b0 <= q < b1 for b0, b1 in BLOCKS) for q in range(NZ)}
    dgot = []

    ring = {}

    def hop(j, to, h):
        part = (lo, hi)[h]
        to = 4 if j == 7 else to
        ring[(to, h)] = start(
            remote(
                zout.at[j, :, part], zin.at[to, :, part], us.at[to, h], ur.at[to, h],
                z_peer(-1) if j in (1, 2, 3) or (j, to) == (4, 3) else z_peer(1),
            )
        )

    def pass_on(j, h):
        part = (lo, hi)[h]
        q = POS[j]
        value = acc[q, :, part]
        if j != 4 and (j, h) not in ((3, 1), (5, 0)):
            ring[(j, h)].wait_recv()
            value = value + zin[j, :, part].astype(F32)
        zout[j, :, part] = value.astype(BF)
        if j == 4:
            hop(j, (3, 5)[h], h)
        elif j < 4:
            hop(j, j - 1, h)
        else:
            hop(j, (j + 1) % NZ, h)

    def gate_terms(chunk):
        spread = jnp.broadcast_to(gsr[...], (NPL, CH, 128))
        value = jnp.sum(jnp.where(lane == row + chunk * CH, spread, 0.0), axis=2, keepdims=True)
        for q in reversed(range(*BLOCKS[chunk])):
            hit = pick(rgo[q, 0:NPL, :].astype(F32), chunk, q)
            i = q - BLOCKS[chunk][0]
            sel = jnp.where(hit, 1.0, 0.0).astype(BF).reshape(NPL * CH, 128)
            px[:, i * 128 : (i + 1) * 128] = sel
            dterm = jnp.sum(jnp.where(hit, value, 0.0), axis=1)
            dsend[q] = dsend[q] + dterm if q in seen else dterm
            seen.add(q)
            left[q] -= 1
            if not left[q] and q:
                j = SEQ[q]
                dgot.append(start(remote(dsend.at[q], dgo.at[j], ds.at[q], dr.at[q], z_peer(-j))))

    def combine(chunk, sem, part, after):
        for cp in rows_back[sem]:
            cp.wait_recv()
        data = ret[chunk, :, :, part].reshape(NPL * CH, part.stop - part.start)
        for q in reversed(range(*BLOCKS[chunk])):
            i = q - BLOCKS[chunk][0]
            sel = px[:, i * 128 : (i + 1) * 128]
            acc[q, :, part] = acc[q, :, part] + dot(sel, data, 0, 0)
            for step in after.get(SEQ[q], ()):
                pass_on(*step)

    full = slice(0, d)
    gate_terms(1)
    combine(1, 1, full, {})
    gate_terms(2)
    combine(2, 2, full, {4: ((4, 0), (4, 1)), 5: ((5, 0),), 3: ((3, 1),)})
    for step in ((3, 0), (5, 1), (2, 1), (6, 0), (2, 0), (6, 1)):
        pass_on(*step)
    gate_terms(0)
    combine(0, 0, lo, {7: ((7, 0),), 1: ((1, 0),)})
    combine(0, NCH, hi, {7: ((7, 1),), 1: ((1, 1),)})
    dgo[0] = dsend[0]
    for cp in part3:
        cp.wait_recv()
    for k in range(3):
        for m in range(NZ // 2):
            pair = [sh3[2 * m + i, k * n : (k + 1) * n, :].astype(F32) for i in range(2)]
            gsho[k, :, m * 2 * n : (m + 1) * 2 * n] = jnp.concatenate(pair, axis=0).T
    save_shared = pltpu.make_async_copy(gsho, gs_hbm, fsem)
    save_shared.start()
    for cp in dgot:
        cp.wait_recv()
    rows = []
    for k in range(ids_ref.shape[0]):
        total = jnp.zeros((NPL, 128), F32)
        for j in range(NZ):
            total = jnp.where(ids_ref[k : k + 1, :] == owners(j), dgo[j], total)
        gate = gw_ref[k : k + 1, :].astype(F32)
        rows.append(jnp.sum(total, axis=0, keepdims=True) / gate)
    ggo[...] = jnp.concatenate(rows, axis=0).astype(BF)
    for h, part in enumerate((lo, hi)):
        ring[(4, h)].wait_recv()
        ring[(0, h)].wait_recv()
        total = acc[0, :, part] + zin[0, :, part].astype(F32) + zin[4, :, part].astype(F32)
        out[:, part] = total.astype(BF)
    save.wait()
    save_shared.wait()
    for cp in sends:
        cp.wait_send()


def layer(xs, ys, ids, gates, weights, shared):
    t, d = xs.shape
    f = weights.shape[3]
    n = shared.shape[2] // NZ
    slots = NCH * NPL * CH
    vm = pl.BlockSpec(memory_space=pltpu.VMEM)
    hbm = pl.BlockSpec(memory_space=pl.ANY)
    dma = pltpu.SemaphoreType.DMA
    v = pltpu.VMEM
    return pl.pallas_call(
        layer_kernel,
        out_shape=(
            jax.ShapeDtypeStruct((t, d), BF),
            jax.ShapeDtypeStruct(gates.shape, BF),
            jax.ShapeDtypeStruct((3, d, f), BF),
            jax.ShapeDtypeStruct((3, 128, NZ * n), F32),
        ),
        in_specs=[hbm, hbm, vm, vm, hbm, hbm],
        out_specs=(vm, vm, hbm, hbm),
        scratch_shapes=[
            v((3, d, f), BF), v((3, d, 2 * n), BF), v((3, d, n), BF), v((3, d, f), BF),
            v((3, 128, NZ * n), F32),
            v((NZ, 2 * NPL, t), BF), v((NZ, NPL, t), F32),
            v((NCH, NPL, CH, d), BF), v((NCH, NPL, CH, d), BF),
            v((NZ, t, d), BF), v((NZ, t, d), BF), v((NZ, 2 * NPL, t), BF),
            v((NCH, NPL, CH, d), BF), v((NCH, NPL, CH, d), BF),
            v((NPL * CH, 512), BF), v((NPL * CH, 512), BF),
            v((slots, f), BF), v((slots, f), BF), v((slots, f), BF),
            v((NCH, NPL, CH, d), BF), v((NCH, NPL, CH, d), BF),
            v((NPL, 1, 128), F32), v((NPL, 1, 128), F32),
            v((NZ, t, d), F32),
            v((3 * n, d), F32), v((3 * n, d), BF),
            v((8, 3 * n, 128), BF), v((4, 3 * n, 128), BF), v((NZ, 3 * n, 128), BF),
            v((NZ, t, d), BF), v((NZ, t, d), BF),
            v((NZ, NPL, t), F32),
            dma, dma, dma, dma, dma, dma,
            dma((2 * NZ,)), dma((2 * NZ,)), dma((NZ,)), dma((NZ,)),
            dma((2, NCH, NPL)), dma((2, NCH, NPL)), dma((NCH + 1, NPL)), dma((NCH + 1, NPL)),
            dma((NPL,)), dma((NPL,)), dma((NZ, 2)), dma((NZ, 2)), dma((NZ,)), dma((NZ,)),
            dma((8,)), dma((8,)), dma((4,)), dma((4,)), dma((NZ,)), dma((NZ,)),
        ],
        compiler_params=pltpu.CompilerParams(
            collective_id=0, has_side_effects=True, vmem_limit_bytes=61 << 20
        ),
        name="layer",
    )(xs, ys, ids, gates, weights, shared)


def finish_kernel(*refs):
    n = 4
    ins, outs, bufs = refs[:n], refs[n : 2 * n], refs[2 * n : 3 * n]
    got, put = refs[3 * n :]
    parts = []
    for i in (2, 3, 0, 1):
        if i >= 2:
            rows = bufs[i].shape[1] // (2 if i == 2 else 1)
            for k in range(bufs[i].shape[0]):
                for r in range(0, bufs[i].shape[1], rows):
                    parts.append((i, (k, slice(r, r + rows))))
        else:
            parts.append((i, (slice(None),)))
    loads = []
    for s, (i, at) in enumerate(parts):
        loads.append(pltpu.make_async_copy(ins[i].at[at], bufs[i].at[at], got.at[s]))
        loads[-1].start()
    stores = []
    for s, (i, at) in enumerate(parts):
        loads[s].wait()
        stores.append(pltpu.make_async_copy(bufs[i].at[at], outs[i].at[at], put.at[s]))
        stores[-1].start()
    for cp in stores:
        cp.wait()


def finish(*arrays):
    hbm = pl.BlockSpec(memory_space=pl.ANY)
    return pl.pallas_call(
        finish_kernel,
        out_shape=tuple(jax.ShapeDtypeStruct(a.shape, a.dtype) for a in arrays),
        in_specs=[hbm] * 4,
        out_specs=(hbm,) * 4,
        scratch_shapes=[pltpu.VMEM(a.shape, a.dtype) for a in arrays]
        + [pltpu.SemaphoreType.DMA((16,)), pltpu.SemaphoreType.DMA((16,))],
        name="finish",
    )(*arrays)


def shards(tokens, cotangent, expert_ids, gate_weights, expert_weights, shared_weights):
    grad_tokens, grad_gates, grad_experts, grad_shared = layer(
        tokens, cotangent, expert_ids.T, gate_weights.T, expert_weights, shared_weights
    )
    grad_tokens, grad_gates, grad_experts, grad_shared = finish(
        grad_tokens, grad_gates, grad_experts, grad_shared
    )
    return (grad_tokens, grad_gates.T, grad_experts[None], grad_shared)


def solution(mesh):
    rows = P(("dp", "expert"), None)
    return jax.shard_map(
        shards,
        mesh=mesh,
        in_specs=(rows, rows, rows, rows, P(("dp", "expert"), None, None, None), P()),
        out_specs=(rows, rows, P(("dp", "expert"), None, None, None), P(None, "dp", None)),
        check_vma=False,
    )
```

```python
import jax
import jax.numpy as jnp
from jax import lax
from jax.experimental import pallas as pl
from jax.experimental.pallas import tpu as pltpu
from jax.sharding import PartitionSpec as P

MESH = pl.DeviceIdType.MESH
BF = jnp.bfloat16
F32 = jnp.float32
NY, NC, NX, NZ = 4, 2, 4, 8
NPL = NY * NC * NX
CAP = 6
CH = 16
NCH = NZ * CAP // CH
SEQ = (0, 1, 7, 2, 6, 3, 5, 4)
POS = {j: q for q, j in enumerate(SEQ)}
BLOCKS = tuple((c * CH // CAP, -(-(c + 1) * CH // CAP)) for c in range(NCH))
ORDER = tuple(
    (i * 8 + c * 4 + (i + j) % 4) for j in range(4) for c in range(2) for i in range(4)
)
ORDER = tuple(o for o in ORDER if o)


def coords():
    d = lax.axis_index("dp")
    e = lax.axis_index("expert")
    return d // 2, d % 2, e % 4, e // 4


def plane_peer(o, sign=1):
    y, c, x, z = coords()
    dy, dc, dx = o // 8, (o // 4) % 2, o % 4
    return (
        lax.rem(y + sign * dy + NY, NY) * 2 + lax.rem(c + dc, NC),
        z * NX + lax.rem(x + sign * dx + NX, NX),
    )


def z_peer(j):
    y, c, x, z = coords()
    return (y * 2 + c, lax.rem(z + j + NZ, NZ) * NX + x)


def owners(j):
    y, c, x, z = coords()
    o = lax.broadcasted_iota(jnp.int32, (NPL, 128), 0)
    dp = lax.rem(y + (o >> 3), NY) * 2 + lax.rem(c + ((o >> 2) & 1), NC)
    return dp * (NZ * NX) + lax.rem(z + j, NZ) * NX + lax.rem(x + (o & 3), NX)


def greet():
    bar = pltpu.get_barrier_semaphore()
    for o in range(1, NPL):
        pl.semaphore_signal(bar, inc=1, device_id=plane_peer(o), device_id_type=MESH)
    for j in range(1, NZ):
        pl.semaphore_signal(bar, inc=1, device_id=z_peer(j), device_id_type=MESH)


def greeted():
    pl.semaphore_wait(pltpu.get_barrier_semaphore(), NPL - 1 + NZ - 1)


def remote(src, dst, ss, rs, dev):
    return pltpu.make_async_remote_copy(
        src_ref=src, dst_ref=dst, send_sem=ss, recv_sem=rs, device_id=dev, device_id_type=MESH
    )


def pick(rank, chunk, q):
    rows = lax.broadcasted_iota(jnp.int32, (NPL, CH, 128), 1) + (chunk * CH - q * CAP)
    return jnp.broadcast_to(rank[:, None, :], (NPL, CH, 128)) == rows.astype(F32)


def dot(a, b, ca, cb):
    return lax.dot_general(a, b, (((ca,), (cb,)), ((), ())), preferred_element_type=F32)


def units(pre_gate, pre_up, back):
    sigma = jax.nn.sigmoid(pre_gate)
    activated = pre_gate * sigma
    slope = sigma * (1.0 + pre_gate * (1.0 - sigma))
    hidden = activated * pre_up
    ggi = (back * pre_up * slope).astype(BF)
    gui = (back * activated).astype(BF)
    return ggi, gui, hidden


def layer_kernel(
    x_hbm, y_hbm, ids_ref, gw_ref, w_hbm, sw_hbm,
    out, ggo, ge_hbm, gs_hbm,
    w, swb, sw_ref, ge, gsho, rg_ref, dgo, rx, ry, xg, yg, rgo, sx, sy, px, pg,
    ggi, gui, hid, dxr, ret, gs, gsr, acc, gsh, gshb, sh1, sh2, sh3, zout, zin, dsend,
    wsem, xsem, ysem, ssem, gsem, fsem, zs, zr, ms, mr, cs, cr, bs, br, gss, grs, us, ur, ds, dr, s1s, s1r, s2s, s2r, s3s, s3r,
):
    y, c, x, z = coords()
    d = x_hbm.shape[1]
    sends = []

    def start(cp):
        cp.start()
        sends.append(cp)
        return cp

    greet()
    own = (
        pltpu.make_async_copy(x_hbm, xg.at[0], xsem),
        pltpu.make_async_copy(y_hbm, yg.at[0], ysem),
    )
    load = pltpu.make_async_copy(w_hbm.at[0], w, wsem)
    halves = pl.ds(pl.multiple_of((z // 2) * 128, 128), 128)
    loads = pltpu.make_async_copy(sw_hbm.at[:, :, halves], swb, ssem)
    own[0].start()
    own[1].start()
    loads.start()
    load.start()
    older = lax.broadcasted_iota(jnp.int32, (128, 128), 0)
    earlier = (older < lax.broadcasted_iota(jnp.int32, (128, 128), 1)).astype(F32).astype(BF)
    for j in range(NZ):
        who = owners(j)
        named = jnp.zeros((NPL, 128), F32)
        gate = jnp.zeros((NPL, 128), F32)
        for k in range(ids_ref.shape[0]):
            hit = ids_ref[k : k + 1, :] == who
            named = jnp.where(hit, 1.0, named)
            gate = jnp.where(hit, gw_ref[k : k + 1, :].astype(F32), gate)
        rank = dot(named.astype(BF), earlier, 1, 0)
        rg_ref[j, 0:NPL, :] = jnp.where(named > 0.5, rank, -100.0).astype(BF)
        rg_ref[j, NPL : 2 * NPL, :] = gate.astype(BF)
    own[0].wait()
    own[1].wait()
    greeted()

    cps = {}
    lo = slice(0, d // 2)
    hi = slice(d // 2, d)

    def go_half(j_to, h):
        part = (lo, hi)[h]
        q = POS[j_to]
        i = 2 * q if h == 0 else (0, 1)[j_to == 7]
        step = 1 if j_to == 1 else -1
        cps[(j_to, 0, h)] = start(
            remote(xg.at[0, :, part], xg.at[q, :, part], zs.at[i], zr.at[i], z_peer(step))
        )

    def go(j_from, j_to, k):
        src = (xg, yg)[k].at[POS[j_from]]
        step = 1 if (j_to - j_from) % NZ == 1 else -1
        i = POS[j_to] * 2 + k
        dst = (xg, yg)[k].at[POS[j_to]]
        cps[(j_to, k)] = start(remote(src, dst, zs.at[i], zr.at[i], z_peer(step)))

    def arrived(*keys):
        for key in keys:
            cps[key].wait_recv()

    metas = []
    for j in range(1, NZ):
        metas.append(
            start(remote(rg_ref.at[j], rgo.at[POS[j]], ms.at[j], mr.at[j], z_peer(j)))
        )
    for h in range(2):
        go_half(1, h)
        go_half(7, h)
    go(0, 1, 1)
    go(0, 7, 1)
    rgo[0] = rg_ref[0]

    for m in metas:
        m.wait_recv()

    rows_in = {chunk: [] for chunk in range(NCH)}

    def choose(chunk, k):
        q0, q1 = BLOCKS[chunk]
        for q in range(q0, q1):
            hit = pick(rgo[q, 0:NPL, :].astype(F32), chunk, q)
            if k:
                gate = rgo[q, NPL : 2 * NPL, :].astype(F32)
                value = jnp.broadcast_to(gate[:, None, :], (NPL, CH, 128))
            else:
                value = 1.0
            lanes = slice((q - q0) * 128, (q - q0 + 1) * 128)
            (px, pg)[k][:, lanes] = jnp.where(hit, value, 0.0).astype(BF).reshape(NPL * CH, 128)

    def pack(chunk, k, part, slot):
        q0, q1 = BLOCKS[chunk]
        width = (q1 - q0) * 128
        cols = part.stop - part.start
        sel, blk, snd, rcv = ((px, xg, sx, rx), (pg, yg, sy, ry))[k]

        def group(g, carry):
            rows = pl.ds(pl.multiple_of(g * 256, 256), 256)
            got = dot(sel[rows, 0:width], blk[q0:q1, :, part].reshape(width, cols), 1, 0)
            os = pl.ds(pl.multiple_of(g * 16, 16), 16)
            snd[chunk, os, :, part] = got.astype(BF).reshape(16, CH, cols)
            return carry

        lax.fori_loop(0, NPL // 16, group, 0)
        rcv[chunk, 0, :, part] = snd[chunk, 0, :, part]
        for o in ORDER:
            sem = (slot, chunk, o)
            rows_in[chunk].append(
                start(
                    remote(
                        snd.at[chunk, o, :, part], rcv.at[chunk, o, :, part],
                        cs.at[sem], cr.at[sem], plane_peer(o),
                    )
                )
            )

    def forward(j_from, j_to, k):
        arrived((j_from, k))
        go(j_from, j_to, k)

    full = slice(0, d)
    choose(0, 0)
    arrived((1, 0, 0), (7, 0, 0))
    pack(0, 0, lo, 0)
    arrived((1, 0, 1))
    go(1, 2, 0)
    arrived((7, 0, 1))
    go(7, 6, 0)
    pack(0, 0, hi, 2)
    choose(0, 1)
    forward(1, 2, 1)
    forward(7, 6, 1)
    pack(0, 1, full, 1)
    for k in range(2):
        forward(2, 3, k)
        forward(6, 5, k)
    forward(3, 4, 0)
    arrived((5, 0))
    choose(1, 0)
    pack(1, 0, full, 0)
    forward(5, 4, 1)
    arrived((3, 1))
    choose(1, 1)
    pack(1, 1, full, 1)
    arrived((4, 0))
    choose(2, 0)
    pack(2, 0, full, 0)
    arrived((4, 1))
    choose(2, 1)
    pack(2, 1, full, 1)

    loads.wait()
    n = swb.shape[2] // 2
    sw_ref[...] = jnp.where(lax.rem(z, 2) == 1, swb[:, :, n:], swb[:, :, :n])
    gsh[...] = jnp.zeros_like(gsh)

    def shared(g, carry):
        two = pl.ds(pl.multiple_of(g * 2, 2), 2)
        bx = xg[two].reshape(256, d)
        by = yg[two].reshape(256, d)
        a, b, hidden = units(
            dot(bx, sw_ref[0], 1, 0), dot(bx, sw_ref[1], 1, 0), dot(by, sw_ref[2], 1, 0)
        )
        n = sw_ref.shape[2]
        acc[two] = (dot(a, sw_ref[0], 1, 1) + dot(b, sw_ref[1], 1, 1)).reshape(2, 128, d)
        gsh[0:n, :] += dot(a, bx, 0, 0)
        gsh[n : 2 * n, :] += dot(b, bx, 0, 0)
        gsh[2 * n : 3 * n, :] += dot(hidden.astype(BF), by, 0, 0)
        return carry

    lax.fori_loop(0, NZ // 2, shared, 0)
    gshb[...] = gsh[...].astype(BF)
    part1 = []
    for i in range(1, 8):
        dev = plane_peer(i * 4)
        src = gshb.at[:, pl.ds(pl.multiple_of(dev[0] * 128, 128), 128)]
        part1.append(start(remote(src, sh1.at[i], s1s.at[i], s1r.at[i], dev)))
    load.wait()

    lane3 = lax.broadcasted_iota(jnp.int32, (16, CH, 128), 2)
    row3 = lax.broadcasted_iota(jnp.int32, (16, CH, 128), 1)

    def expert(chunk):
        for cp in rows_in[chunk]:
            cp.wait_recv()

        def group(g, carry):
            os = pl.ds(pl.multiple_of(g * 16, 16), 16)
            rs = pl.ds(pl.multiple_of(chunk * 512 + g * 256, 256), 256)
            bx = rx[chunk, os].reshape(256, d)
            by = ry[chunk, os].reshape(256, d)
            back = dot(by, w[2], 1, 0)
            a, b, hidden = units(dot(bx, w[0], 1, 0), dot(bx, w[1], 1, 0), back)
            ggi[rs, :] = a
            gui[rs, :] = b
            hid[rs, :] = hidden.astype(BF)
            gg = jnp.sum(hidden * back, axis=1, keepdims=True).reshape(16, CH, 1)
            term = jnp.where(lane3 == row3 + chunk * CH, gg, 0.0)
            term = jnp.sum(term, axis=1, keepdims=True)
            if chunk == 0:
                gs[os] = term
            else:
                gs[os] = gs[os] + term
            grads = dot(a, w[0], 1, 1) + dot(b, w[1], 1, 1)
            dxr[chunk, os] = grads.astype(BF).reshape(16, CH, d)
            return carry

        lax.fori_loop(0, 2, group, 0)

    rows_back = {}

    def give_back(chunk, sem, part):
        got = []
        for o in ORDER:
            got.append(
                start(
                    remote(
                        dxr.at[chunk, o, :, part], ret.at[chunk, o, :, part],
                        bs.at[sem, o], br.at[sem, o], plane_peer(o, -1),
                    )
                )
            )
        rows_back[sem] = got

    expert(0)
    expert(1)
    give_back(1, 1, slice(0, d))
    expert(2)
    for cp in part1:
        cp.wait_recv()
    mine = pl.ds(pl.multiple_of((y * 2 + c) * 128, 128), 128)
    total = gsh[:, mine]
    for i in range(1, 8):
        total = total + sh1[i].astype(F32)
    sh2[0] = total.astype(BF)
    part2 = []
    for o in (1, 3, 2):
        part2.append(start(remote(sh2.at[0], sh2.at[o], s2s.at[o], s2r.at[o], plane_peer(o))))
    gates = []
    for o in ORDER:
        gates.append(start(remote(gs.at[o], gsr.at[o], gss.at[o], grs.at[o], plane_peer(o, -1))))
    gsr[0] = gs[0]
    give_back(2, 2, slice(0, d))
    give_back(0, 0, lo)
    give_back(0, NCH, hi)
    for chunk in range(NCH):
        ret[chunk, 0] = dxr[chunk, 0]

    def wgrad(g, carry):
        cols = pl.ds(pl.multiple_of(g * 256, 256), 256)
        bx = rx[:, :, :, cols].reshape(NCH * NPL * CH, 256)
        ge[0, cols, :] = dot(bx, ggi[...], 0, 0).astype(BF)
        ge[1, cols, :] = dot(bx, gui[...], 0, 0).astype(BF)
        by = ry[:, :, :, cols].reshape(NCH * NPL * CH, 256)
        ge[2, cols, :] = dot(by, hid[...], 0, 0).astype(BF)
        return carry

    lax.fori_loop(0, d // 256, wgrad, 0)
    save = pltpu.make_async_copy(ge, ge_hbm, gsem)
    save.start()

    for cp in part2:
        cp.wait_recv()
    total = sh2[0].astype(F32)
    for o in range(1, 4):
        total = total + sh2[o].astype(F32)
    sh3[z] = total.astype(BF)
    part3 = []
    for j in (1, 7, 2, 6, 3, 5, 4):
        part3.append(start(remote(sh3.at[z], sh3.at[z], s3s.at[j], s3r.at[j], z_peer(j))))

    lane = lax.broadcasted_iota(jnp.int32, (NPL, CH, 128), 2)
    row = lax.broadcasted_iota(jnp.int32, (NPL, CH, 128), 1)
    for cp in gates:
        cp.wait_recv()
    seen = set()
    left = {q: sum(b0 <= q < b1 for b0, b1 in BLOCKS) for q in range(NZ)}
    dgot = []

    ring = {}
    parts = [slice(h * d // 4, (h + 1) * d // 4) for h in range(4)]

    def hop(j, to, h):
        part = parts[h]
        to = 4 if j == 7 else to
        ring[(to, h)] = start(
            remote(
                zout.at[j, :, part], zin.at[to, :, part], us.at[to, h], ur.at[to, h],
                z_peer(-1) if j in (1, 2, 3) or (j, to) == (4, 3) else z_peer(1),
            )
        )

    def pass_on(j, h):
        part = parts[h]
        q = POS[j]
        value = acc[q, :, part]
        if j != 4 and (j, h) not in ((3, 2), (3, 3), (5, 0), (5, 1)):
            ring[(j, h)].wait_recv()
            value = value + zin[j, :, part].astype(F32)
        zout[j, :, part] = value.astype(BF)
        if j == 4:
            hop(j, (3, 5)[h // 2], h)
        elif j < 4:
            hop(j, j - 1, h)
        else:
            hop(j, (j + 1) % NZ, h)

    def gate_terms(chunk, keep):
        spread = jnp.broadcast_to(gsr[...], (NPL, CH, 128))
        value = jnp.sum(jnp.where(lane == row + chunk * CH, spread, 0.0), axis=2, keepdims=True)
        for q in reversed(range(*BLOCKS[chunk])):
            hit = pick(rgo[q, 0:NPL, :].astype(F32), chunk, q)
            i = q - BLOCKS[chunk][0]
            sel = jnp.where(hit, 1.0, 0.0).astype(BF).reshape(NPL * CH, 128)
            keep[:, i * 128 : (i + 1) * 128] = sel
            dterm = jnp.sum(jnp.where(hit, value, 0.0), axis=1)
            dsend[q] = dsend[q] + dterm if q in seen else dterm
            seen.add(q)
            left[q] -= 1
            if not left[q] and q:
                j = SEQ[q]
                dgot.append(start(remote(dsend.at[q], dgo.at[j], ds.at[q], dr.at[q], z_peer(-j))))

    def combine(chunk, sem, keep, part, after):
        for cp in rows_back[sem]:
            cp.wait_recv()
        data = ret[chunk, :, :, part].reshape(NPL * CH, part.stop - part.start)
        for q in reversed(range(*BLOCKS[chunk])):
            i = q - BLOCKS[chunk][0]
            sel = keep[:, i * 128 : (i + 1) * 128]
            acc[q, :, part] = acc[q, :, part] + dot(sel, data, 0, 0)
            for step in after.get(SEQ[q], ()):
                pass_on(*step)

    gate_terms(1, px)
    gate_terms(2, pg)
    combine(1, 1, px, full, {})
    gate_terms(0, px)
    combine(
        2, 2, pg, full,
        {
            4: ((4, 0), (4, 2), (4, 1), (4, 3)),
            5: ((5, 0), (5, 1)),
            3: ((3, 2), (3, 3)),
        },
    )
    for step in ((3, 0), (5, 2), (3, 1), (5, 3), (2, 2), (6, 0), (2, 3), (6, 1)):
        pass_on(*step)
    for step in ((2, 0), (6, 2), (2, 1), (6, 3)):
        pass_on(*step)
    combine(0, 0, px, lo, {7: ((7, 0), (7, 1)), 1: ((1, 0), (1, 1))})
    combine(0, NCH, px, hi, {7: ((7, 2), (7, 3)), 1: ((1, 2), (1, 3))})
    dgo[0] = dsend[0]
    for cp in part3:
        cp.wait_recv()
    for k in range(3):
        for m in range(NZ // 2):
            pair = [sh3[2 * m + i, k * n : (k + 1) * n, :].astype(F32) for i in range(2)]
            gsho[k, :, m * 2 * n : (m + 1) * 2 * n] = jnp.concatenate(pair, axis=0).T
    save_shared = pltpu.make_async_copy(gsho, gs_hbm, fsem)
    save_shared.start()
    for cp in dgot:
        cp.wait_recv()
    rows = []
    for k in range(ids_ref.shape[0]):
        total = jnp.zeros((NPL, 128), F32)
        for j in range(NZ):
            total = jnp.where(ids_ref[k : k + 1, :] == owners(j), dgo[j], total)
        gate = gw_ref[k : k + 1, :].astype(F32)
        rows.append(jnp.sum(total, axis=0, keepdims=True) / gate)
    ggo[...] = jnp.concatenate(rows, axis=0).astype(BF)
    for h, part in enumerate(parts):
        ring[(4, h)].wait_recv()
        ring[(0, h)].wait_recv()
        total = acc[0, :, part] + zin[0, :, part].astype(F32) + zin[4, :, part].astype(F32)
        out[:, part] = total.astype(BF)
    save.wait()
    save_shared.wait()
    for cp in sends:
        cp.wait_send()


def layer(xs, ys, ids, gates, weights, shared):
    t, d = xs.shape
    f = weights.shape[3]
    n = shared.shape[2] // NZ
    slots = NCH * NPL * CH
    vm = pl.BlockSpec(memory_space=pltpu.VMEM)
    hbm = pl.BlockSpec(memory_space=pl.ANY)
    dma = pltpu.SemaphoreType.DMA
    v = pltpu.VMEM
    return pl.pallas_call(
        layer_kernel,
        out_shape=(
            jax.ShapeDtypeStruct((t, d), BF),
            jax.ShapeDtypeStruct(gates.shape, BF),
            jax.ShapeDtypeStruct((3, d, f), BF),
            jax.ShapeDtypeStruct((3, 128, NZ * n), F32),
        ),
        in_specs=[hbm, hbm, vm, vm, hbm, hbm],
        out_specs=(vm, vm, hbm, hbm),
        scratch_shapes=[
            v((3, d, f), BF), v((3, d, 2 * n), BF), v((3, d, n), BF), v((3, d, f), BF),
            v((3, 128, NZ * n), F32),
            v((NZ, 2 * NPL, t), BF), v((NZ, NPL, t), F32),
            v((NCH, NPL, CH, d), BF), v((NCH, NPL, CH, d), BF),
            v((NZ, t, d), BF), v((NZ, t, d), BF), v((NZ, 2 * NPL, t), BF),
            v((NCH, NPL, CH, d), BF), v((NCH, NPL, CH, d), BF),
            v((NPL * CH, 512), BF), v((NPL * CH, 512), BF),
            v((slots, f), BF), v((slots, f), BF), v((slots, f), BF),
            v((NCH, NPL, CH, d), BF), v((NCH, NPL, CH, d), BF),
            v((NPL, 1, 128), F32), v((NPL, 1, 128), F32),
            v((NZ, t, d), F32),
            v((3 * n, d), F32), v((3 * n, d), BF),
            v((8, 3 * n, 128), BF), v((4, 3 * n, 128), BF), v((NZ, 3 * n, 128), BF),
            v((NZ, t, d), BF), v((NZ, t, d), BF),
            v((NZ, NPL, t), F32),
            dma, dma, dma, dma, dma, dma,
            dma((2 * NZ,)), dma((2 * NZ,)), dma((NZ,)), dma((NZ,)),
            dma((3, NCH, NPL)), dma((3, NCH, NPL)), dma((NCH + 1, NPL)), dma((NCH + 1, NPL)),
            dma((NPL,)), dma((NPL,)), dma((NZ, 4)), dma((NZ, 4)), dma((NZ,)), dma((NZ,)),
            dma((8,)), dma((8,)), dma((4,)), dma((4,)), dma((NZ,)), dma((NZ,)),
        ],
        compiler_params=pltpu.CompilerParams(
            collective_id=0, has_side_effects=True, vmem_limit_bytes=61 << 20
        ),
        name="layer",
    )(xs, ys, ids, gates, weights, shared)


def finish_kernel(*refs):
    n = 4
    ins, outs, bufs = refs[:n], refs[n : 2 * n], refs[2 * n : 3 * n]
    got, put = refs[3 * n :]
    parts = []
    for i in (2, 3, 0, 1):
        if i >= 2:
            rows = bufs[i].shape[1] // (2 if i == 2 else 1)
            for k in range(bufs[i].shape[0]):
                for r in range(0, bufs[i].shape[1], rows):
                    parts.append((i, (k, slice(r, r + rows))))
        else:
            parts.append((i, (slice(None),)))
    loads = []
    for s, (i, at) in enumerate(parts):
        loads.append(pltpu.make_async_copy(ins[i].at[at], bufs[i].at[at], got.at[s]))
        loads[-1].start()
    stores = []
    for s, (i, at) in enumerate(parts):
        loads[s].wait()
        stores.append(pltpu.make_async_copy(bufs[i].at[at], outs[i].at[at], put.at[s]))
        stores[-1].start()
    for cp in stores:
        cp.wait()


def finish(*arrays):
    hbm = pl.BlockSpec(memory_space=pl.ANY)
    return pl.pallas_call(
        finish_kernel,
        out_shape=tuple(jax.ShapeDtypeStruct(a.shape, a.dtype) for a in arrays),
        in_specs=[hbm] * 4,
        out_specs=(hbm,) * 4,
        scratch_shapes=[pltpu.VMEM(a.shape, a.dtype) for a in arrays]
        + [pltpu.SemaphoreType.DMA((16,)), pltpu.SemaphoreType.DMA((16,))],
        name="finish",
    )(*arrays)


def shards(tokens, cotangent, expert_ids, gate_weights, expert_weights, shared_weights):
    grad_tokens, grad_gates, grad_experts, grad_shared = layer(
        tokens, cotangent, expert_ids.T, gate_weights.T, expert_weights, shared_weights
    )
    grad_tokens, grad_gates, grad_experts, grad_shared = finish(
        grad_tokens, grad_gates, grad_experts, grad_shared
    )
    return (grad_tokens, grad_gates.T, grad_experts[None], grad_shared)


def solution(mesh):
    rows = P(("dp", "expert"), None)
    return jax.shard_map(
        shards,
        mesh=mesh,
        in_specs=(rows, rows, rows, rows, P(("dp", "expert"), None, None, None), P()),
        out_specs=(rows, rows, P(("dp", "expert"), None, None, None), P(None, "dp", None)),
        check_vma=False,
    )
```

```python
import jax
import jax.numpy as jnp
from jax import lax
from jax.experimental import pallas as pl
from jax.experimental.pallas import tpu as pltpu
from jax.sharding import PartitionSpec as P

MESH = pl.DeviceIdType.MESH
BF = jnp.bfloat16
F32 = jnp.float32
NY, NC, NX, NZ = 4, 2, 4, 8
NPL = NY * NC * NX
CAP = 6
CH = 16
NCH = NZ * CAP // CH
SEQ = (0, 1, 7, 2, 6, 3, 5, 4)
POS = {j: q for q, j in enumerate(SEQ)}
BLOCKS = tuple((c * CH // CAP, -(-(c + 1) * CH // CAP)) for c in range(NCH))
ORDER = tuple(
    (i * 8 + c * 4 + (i + j) % 4) for j in range(4) for c in range(2) for i in range(4)
)
ORDER = tuple(o for o in ORDER if o)


def coords():
    d = lax.axis_index("dp")
    e = lax.axis_index("expert")
    return d // 2, d % 2, e % 4, e // 4


def plane_peer(o, sign=1):
    y, c, x, z = coords()
    dy, dc, dx = o // 8, (o // 4) % 2, o % 4
    return (
        lax.rem(y + sign * dy + NY, NY) * 2 + lax.rem(c + dc, NC),
        z * NX + lax.rem(x + sign * dx + NX, NX),
    )


def z_peer(j):
    y, c, x, z = coords()
    return (y * 2 + c, lax.rem(z + j + NZ, NZ) * NX + x)


def owners(j):
    y, c, x, z = coords()
    o = lax.broadcasted_iota(jnp.int32, (NPL, 128), 0)
    dp = lax.rem(y + (o >> 3), NY) * 2 + lax.rem(c + ((o >> 2) & 1), NC)
    return dp * (NZ * NX) + lax.rem(z + j, NZ) * NX + lax.rem(x + (o & 3), NX)


def greet():
    bar = pltpu.get_barrier_semaphore()
    for o in range(1, NPL):
        pl.semaphore_signal(bar, inc=1, device_id=plane_peer(o), device_id_type=MESH)
    for j in range(1, NZ):
        pl.semaphore_signal(bar, inc=1, device_id=z_peer(j), device_id_type=MESH)


def greeted():
    pl.semaphore_wait(pltpu.get_barrier_semaphore(), NPL - 1 + NZ - 1)


def remote(src, dst, ss, rs, dev):
    return pltpu.make_async_remote_copy(
        src_ref=src, dst_ref=dst, send_sem=ss, recv_sem=rs, device_id=dev, device_id_type=MESH
    )


def pick(rank, chunk, q):
    rows = lax.broadcasted_iota(jnp.int32, (NPL, CH, 128), 1) + (chunk * CH - q * CAP)
    return jnp.broadcast_to(rank[:, None, :], (NPL, CH, 128)) == rows.astype(F32)


def dot(a, b, ca, cb):
    return lax.dot_general(a, b, (((ca,), (cb,)), ((), ())), preferred_element_type=F32)


def units(pre_gate, pre_up, back):
    sigma = jax.nn.sigmoid(pre_gate)
    activated = pre_gate * sigma
    slope = sigma * (1.0 + pre_gate * (1.0 - sigma))
    hidden = activated * pre_up
    ggi = (back * pre_up * slope).astype(BF)
    gui = (back * activated).astype(BF)
    return ggi, gui, hidden


def layer_kernel(
    x_hbm, y_hbm, ids_ref, gw_ref, w_hbm, sw_hbm,
    out, ggo, ge_hbm, gs_hbm,
    w, swb, sw_ref, ge, gsho, rg_ref, dgo, rx, ry, xg, yg, rgo, sx, sy, px, pg,
    ggi, gui, hid, dxr, ret, gs, gsr, acc, gsh, gshb, sh1, sh2, sh3, zout, zin, dsend,
    wsem, xsem, ysem, ssem, gsem, fsem, zs, zr, ms, mr, cs, cr, bs, br, gss, grs, us, ur, ds, dr, s1s, s1r, s2s, s2r, s3s, s3r,
):
    y, c, x, z = coords()
    d = x_hbm.shape[1]
    sends = []

    def start(cp):
        cp.start()
        sends.append(cp)
        return cp

    greet()
    own = (
        pltpu.make_async_copy(x_hbm, xg.at[0], xsem),
        pltpu.make_async_copy(y_hbm, yg.at[0], ysem),
    )
    load = pltpu.make_async_copy(w_hbm.at[0], w, wsem)
    halves = pl.ds(pl.multiple_of((z // 2) * 128, 128), 128)
    loads = pltpu.make_async_copy(sw_hbm.at[:, :, halves], swb, ssem)
    own[0].start()
    own[1].start()
    loads.start()
    load.start()
    older = lax.broadcasted_iota(jnp.int32, (128, 128), 0)
    earlier = (older < lax.broadcasted_iota(jnp.int32, (128, 128), 1)).astype(F32).astype(BF)
    for j in range(NZ):
        who = owners(j)
        named = jnp.zeros((NPL, 128), F32)
        gate = jnp.zeros((NPL, 128), F32)
        for k in range(ids_ref.shape[0]):
            hit = ids_ref[k : k + 1, :] == who
            named = jnp.where(hit, 1.0, named)
            gate = jnp.where(hit, gw_ref[k : k + 1, :].astype(F32), gate)
        rank = dot(named.astype(BF), earlier, 1, 0)
        rg_ref[j, 0:NPL, :] = jnp.where(named > 0.5, rank, -100.0).astype(BF)
        rg_ref[j, NPL : 2 * NPL, :] = gate.astype(BF)
    own[0].wait()
    own[1].wait()
    greeted()

    cps = {}

    def go(j_from, j_to, k):
        src = (xg, yg)[k].at[POS[j_from]]
        step = 1 if (j_to - j_from) % NZ == 1 else -1
        i = POS[j_to] * 2 + k
        dst = (xg, yg)[k].at[POS[j_to]]
        cps[(j_to, k)] = start(remote(src, dst, zs.at[i], zr.at[i], z_peer(step)))

    def arrived(*keys):
        for key in keys:
            cps[key].wait_recv()

    metas = []
    for j in range(1, NZ):
        metas.append(
            start(remote(rg_ref.at[j], rgo.at[POS[j]], ms.at[j], mr.at[j], z_peer(j)))
        )
    for k in range(2):
        go(0, 1, k)
        go(0, 7, k)
    rgo[0] = rg_ref[0]

    for m in metas:
        m.wait_recv()

    rows_in = {chunk: [] for chunk in range(NCH)}

    def pack(chunk, k):
        q0, q1 = BLOCKS[chunk]
        width = (q1 - q0) * 128
        sel, blk, snd, rcv = ((px, xg, sx, rx), (pg, yg, sy, ry))[k]
        for q in range(q0, q1):
            hit = pick(rgo[q, 0:NPL, :].astype(F32), chunk, q)
            if k:
                gate = rgo[q, NPL : 2 * NPL, :].astype(F32)
                value = jnp.broadcast_to(gate[:, None, :], (NPL, CH, 128))
            else:
                value = 1.0
            lanes = slice((q - q0) * 128, (q - q0 + 1) * 128)
            sel[:, lanes] = jnp.where(hit, value, 0.0).astype(BF).reshape(NPL * CH, 128)

        def group(g, carry):
            rows = pl.ds(pl.multiple_of(g * 256, 256), 256)
            got = dot(sel[rows, 0:width], blk[q0:q1].reshape(width, d), 1, 0)
            os = pl.ds(pl.multiple_of(g * 16, 16), 16)
            snd[chunk, os] = got.astype(BF).reshape(16, CH, d)
            return carry

        lax.fori_loop(0, NPL // 16, group, 0)
        rcv[chunk, 0] = snd[chunk, 0]
        for o in ORDER:
            sem = (k, chunk, o)
            rows_in[chunk].append(
                start(
                    remote(
                        snd.at[chunk, o], rcv.at[chunk, o], cs.at[sem], cr.at[sem], plane_peer(o)
                    )
                )
            )

    def forward(j_from, j_to, k):
        arrived((j_from, k))
        go(j_from, j_to, k)

    for k in range(2):
        forward(1, 2, k)
        forward(7, 6, k)
        pack(0, k)
    for k in range(2):
        forward(2, 3, k)
        forward(6, 5, k)
    forward(3, 4, 0)
    arrived((5, 0))
    pack(1, 0)
    forward(5, 4, 1)
    arrived((3, 1))
    pack(1, 1)
    arrived((4, 0))
    pack(2, 0)
    arrived((4, 1))
    pack(2, 1)

    loads.wait()
    n = swb.shape[2] // 2
    sw_ref[...] = jnp.where(lax.rem(z, 2) == 1, swb[:, :, n:], swb[:, :, :n])
    gsh[...] = jnp.zeros_like(gsh)

    def shared(g, carry):
        two = pl.ds(pl.multiple_of(g * 2, 2), 2)
        bx = xg[two].reshape(256, d)
        by = yg[two].reshape(256, d)
        a, b, hidden = units(
            dot(bx, sw_ref[0], 1, 0), dot(bx, sw_ref[1], 1, 0), dot(by, sw_ref[2], 1, 0)
        )
        n = sw_ref.shape[2]
        acc[two] = (dot(a, sw_ref[0], 1, 1) + dot(b, sw_ref[1], 1, 1)).reshape(2, 128, d)
        gsh[0:n, :] += dot(a, bx, 0, 0)
        gsh[n : 2 * n, :] += dot(b, bx, 0, 0)
        gsh[2 * n : 3 * n, :] += dot(hidden.astype(BF), by, 0, 0)
        return carry

    lax.fori_loop(0, NZ // 2, shared, 0)
    gshb[...] = gsh[...].astype(BF)
    part1 = []
    for i in range(1, 8):
        dev = plane_peer(i * 4)
        src = gshb.at[:, pl.ds(pl.multiple_of(dev[0] * 128, 128), 128)]
        part1.append(start(remote(src, sh1.at[i], s1s.at[i], s1r.at[i], dev)))
    load.wait()

    lane3 = lax.broadcasted_iota(jnp.int32, (16, CH, 128), 2)
    row3 = lax.broadcasted_iota(jnp.int32, (16, CH, 128), 1)

    def expert(chunk):
        for cp in rows_in[chunk]:
            cp.wait_recv()

        def group(g, carry):
            os = pl.ds(pl.multiple_of(g * 16, 16), 16)
            rs = pl.ds(pl.multiple_of(chunk * 512 + g * 256, 256), 256)
            bx = rx[chunk, os].reshape(256, d)
            by = ry[chunk, os].reshape(256, d)
            back = dot(by, w[2], 1, 0)
            a, b, hidden = units(dot(bx, w[0], 1, 0), dot(bx, w[1], 1, 0), back)
            ggi[rs, :] = a
            gui[rs, :] = b
            hid[rs, :] = hidden.astype(BF)
            gg = jnp.sum(hidden * back, axis=1, keepdims=True).reshape(16, CH, 1)
            term = jnp.where(lane3 == row3 + chunk * CH, gg, 0.0)
            term = jnp.sum(term, axis=1, keepdims=True)
            if chunk == 0:
                gs[os] = term
            else:
                gs[os] = gs[os] + term
            grads = dot(a, w[0], 1, 1) + dot(b, w[1], 1, 1)
            dxr[chunk, os] = grads.astype(BF).reshape(16, CH, d)
            return carry

        lax.fori_loop(0, 2, group, 0)

    rows_back = {}

    lo = slice(0, d // 2)
    hi = slice(d // 2, d)

    def give_back(chunk, sem, part):
        got = []
        for o in ORDER:
            got.append(
                start(
                    remote(
                        dxr.at[chunk, o, :, part], ret.at[chunk, o, :, part],
                        bs.at[sem, o], br.at[sem, o], plane_peer(o, -1),
                    )
                )
            )
        rows_back[sem] = got

    expert(0)
    expert(1)
    give_back(1, 1, slice(0, d))
    expert(2)
    for cp in part1:
        cp.wait_recv()
    mine = pl.ds(pl.multiple_of((y * 2 + c) * 128, 128), 128)
    total = gsh[:, mine]
    for i in range(1, 8):
        total = total + sh1[i].astype(F32)
    sh2[0] = total.astype(BF)
    part2 = []
    for o in (1, 3, 2):
        part2.append(start(remote(sh2.at[0], sh2.at[o], s2s.at[o], s2r.at[o], plane_peer(o))))
    gates = []
    for o in ORDER:
        gates.append(start(remote(gs.at[o], gsr.at[o], gss.at[o], grs.at[o], plane_peer(o, -1))))
    gsr[0] = gs[0]
    give_back(2, 2, slice(0, d))
    give_back(0, 0, lo)
    give_back(0, NCH, hi)
    for chunk in range(NCH):
        ret[chunk, 0] = dxr[chunk, 0]

    def wgrad(g, carry):
        cols = pl.ds(pl.multiple_of(g * 256, 256), 256)
        bx = rx[:, :, :, cols].reshape(NCH * NPL * CH, 256)
        ge[0, cols, :] = dot(bx, ggi[...], 0, 0).astype(BF)
        ge[1, cols, :] = dot(bx, gui[...], 0, 0).astype(BF)
        by = ry[:, :, :, cols].reshape(NCH * NPL * CH, 256)
        ge[2, cols, :] = dot(by, hid[...], 0, 0).astype(BF)
        return carry

    lax.fori_loop(0, d // 512, wgrad, 0)

    for cp in part2:
        cp.wait_recv()
    total = sh2[0].astype(F32)
    for o in range(1, 4):
        total = total + sh2[o].astype(F32)
    sh3[z] = total.astype(BF)
    part3 = []
    for j in (1, 7, 2, 6, 3, 5, 4):
        part3.append(start(remote(sh3.at[z], sh3.at[z], s3s.at[j], s3r.at[j], z_peer(j))))

    lane = lax.broadcasted_iota(jnp.int32, (NPL, CH, 128), 2)
    row = lax.broadcasted_iota(jnp.int32, (NPL, CH, 128), 1)
    for cp in gates:
        cp.wait_recv()
    seen = set()
    left = {q: sum(b0 <= q < b1 for b0, b1 in BLOCKS) for q in range(NZ)}
    dgot = []

    ring = {}

    def hop(j, to, h):
        part = (lo, hi)[h]
        to = 4 if j == 7 else to
        ring[(to, h)] = start(
            remote(
                zout.at[j, :, part], zin.at[to, :, part], us.at[to, h], ur.at[to, h],
                z_peer(-1) if j in (1, 2, 3) or (j, to) == (4, 3) else z_peer(1),
            )
        )

    def pass_on(j, h):
        part = (lo, hi)[h]
        q = POS[j]
        value = acc[q, :, part]
        if j != 4 and (j, h) not in ((3, 1), (5, 0)):
            ring[(j, h)].wait_recv()
            value = value + zin[j, :, part].astype(F32)
        zout[j, :, part] = value.astype(BF)
        if j == 4:
            hop(j, (3, 5)[h], h)
        elif j < 4:
            hop(j, j - 1, h)
        else:
            hop(j, (j + 1) % NZ, h)

    def gate_terms(chunk):
        spread = jnp.broadcast_to(gsr[...], (NPL, CH, 128))
        value = jnp.sum(jnp.where(lane == row + chunk * CH, spread, 0.0), axis=2, keepdims=True)
        for q in reversed(range(*BLOCKS[chunk])):
            hit = pick(rgo[q, 0:NPL, :].astype(F32), chunk, q)
            i = q - BLOCKS[chunk][0]
            sel = jnp.where(hit, 1.0, 0.0).astype(BF).reshape(NPL * CH, 128)
            px[:, i * 128 : (i + 1) * 128] = sel
            dterm = jnp.sum(jnp.where(hit, value, 0.0), axis=1)
            dsend[q] = dsend[q] + dterm if q in seen else dterm
            seen.add(q)
            left[q] -= 1
            if not left[q] and q:
                j = SEQ[q]
                dgot.append(start(remote(dsend.at[q], dgo.at[j], ds.at[q], dr.at[q], z_peer(-j))))

    def combine(chunk, sem, part, after):
        for cp in rows_back[sem]:
            cp.wait_recv()
        data = ret[chunk, :, :, part].reshape(NPL * CH, part.stop - part.start)
        for q in reversed(range(*BLOCKS[chunk])):
            i = q - BLOCKS[chunk][0]
            sel = px[:, i * 128 : (i + 1) * 128]
            acc[q, :, part] = acc[q, :, part] + dot(sel, data, 0, 0)
            for step in after.get(SEQ[q], ()):
                pass_on(*step)

    full = slice(0, d)
    gate_terms(1)
    combine(1, 1, full, {})
    gate_terms(2)
    combine(2, 2, full, {4: ((4, 0), (4, 1)), 5: ((5, 0),), 3: ((3, 1),)})
    lax.fori_loop(d // 512, d // 512 + 1, wgrad, 0)
    for step in ((3, 0), (5, 1), (2, 1), (6, 0)):
        pass_on(*step)
    lax.fori_loop(d // 512 + 1, d // 256, wgrad, 0)
    save = pltpu.make_async_copy(ge, ge_hbm, gsem)
    save.start()
    for step in ((2, 0), (6, 1)):
        pass_on(*step)
    gate_terms(0)
    combine(0, 0, lo, {7: ((7, 0),), 1: ((1, 0),)})
    combine(0, NCH, hi, {7: ((7, 1),), 1: ((1, 1),)})
    dgo[0] = dsend[0]
    for cp in part3:
        cp.wait_recv()
    for k in range(3):
        for m in range(NZ // 2):
            pair = [sh3[2 * m + i, k * n : (k + 1) * n, :].astype(F32) for i in range(2)]
            gsho[k, :, m * 2 * n : (m + 1) * 2 * n] = jnp.concatenate(pair, axis=0).T
    save_shared = pltpu.make_async_copy(gsho, gs_hbm, fsem)
    save_shared.start()
    for cp in dgot:
        cp.wait_recv()
    rows = []
    for k in range(ids_ref.shape[0]):
        total = jnp.zeros((NPL, 128), F32)
        for j in range(NZ):
            total = jnp.where(ids_ref[k : k + 1, :] == owners(j), dgo[j], total)
        gate = gw_ref[k : k + 1, :].astype(F32)
        rows.append(jnp.sum(total, axis=0, keepdims=True) / gate)
    ggo[...] = jnp.concatenate(rows, axis=0).astype(BF)
    for h, part in enumerate((lo, hi)):
        ring[(4, h)].wait_recv()
        ring[(0, h)].wait_recv()
        total = acc[0, :, part] + zin[0, :, part].astype(F32) + zin[4, :, part].astype(F32)
        out[:, part] = total.astype(BF)
    save.wait()
    save_shared.wait()
    for cp in sends:
        cp.wait_send()


def layer(xs, ys, ids, gates, weights, shared):
    t, d = xs.shape
    f = weights.shape[3]
    n = shared.shape[2] // NZ
    slots = NCH * NPL * CH
    vm = pl.BlockSpec(memory_space=pltpu.VMEM)
    hbm = pl.BlockSpec(memory_space=pl.ANY)
    dma = pltpu.SemaphoreType.DMA
    v = pltpu.VMEM
    return pl.pallas_call(
        layer_kernel,
        out_shape=(
            jax.ShapeDtypeStruct((t, d), BF),
            jax.ShapeDtypeStruct(gates.shape, BF),
            jax.ShapeDtypeStruct((3, d, f), BF),
            jax.ShapeDtypeStruct((3, 128, NZ * n), F32),
        ),
        in_specs=[hbm, hbm, vm, vm, hbm, hbm],
        out_specs=(vm, vm, hbm, hbm),
        scratch_shapes=[
            v((3, d, f), BF), v((3, d, 2 * n), BF), v((3, d, n), BF), v((3, d, f), BF),
            v((3, 128, NZ * n), F32),
            v((NZ, 2 * NPL, t), BF), v((NZ, NPL, t), F32),
            v((NCH, NPL, CH, d), BF), v((NCH, NPL, CH, d), BF),
            v((NZ, t, d), BF), v((NZ, t, d), BF), v((NZ, 2 * NPL, t), BF),
            v((NCH, NPL, CH, d), BF), v((NCH, NPL, CH, d), BF),
            v((NPL * CH, 512), BF), v((NPL * CH, 512), BF),
            v((slots, f), BF), v((slots, f), BF), v((slots, f), BF),
            v((NCH, NPL, CH, d), BF), v((NCH, NPL, CH, d), BF),
            v((NPL, 1, 128), F32), v((NPL, 1, 128), F32),
            v((NZ, t, d), F32),
            v((3 * n, d), F32), v((3 * n, d), BF),
            v((8, 3 * n, 128), BF), v((4, 3 * n, 128), BF), v((NZ, 3 * n, 128), BF),
            v((NZ, t, d), BF), v((NZ, t, d), BF),
            v((NZ, NPL, t), F32),
            dma, dma, dma, dma, dma, dma,
            dma((2 * NZ,)), dma((2 * NZ,)), dma((NZ,)), dma((NZ,)),
            dma((2, NCH, NPL)), dma((2, NCH, NPL)), dma((NCH + 1, NPL)), dma((NCH + 1, NPL)),
            dma((NPL,)), dma((NPL,)), dma((NZ, 2)), dma((NZ, 2)), dma((NZ,)), dma((NZ,)),
            dma((8,)), dma((8,)), dma((4,)), dma((4,)), dma((NZ,)), dma((NZ,)),
        ],
        compiler_params=pltpu.CompilerParams(
            collective_id=0, has_side_effects=True, vmem_limit_bytes=61 << 20
        ),
        name="layer",
    )(xs, ys, ids, gates, weights, shared)


def finish_kernel(*refs):
    n = 4
    ins, outs, bufs = refs[:n], refs[n : 2 * n], refs[2 * n : 3 * n]
    got, put = refs[3 * n :]
    parts = []
    for i in (2, 3, 0, 1):
        if i >= 2:
            rows = bufs[i].shape[1] // (2 if i == 2 else 1)
            for k in range(bufs[i].shape[0]):
                for r in range(0, bufs[i].shape[1], rows):
                    parts.append((i, (k, slice(r, r + rows))))
        else:
            parts.append((i, (slice(None),)))
    loads = []
    for s, (i, at) in enumerate(parts):
        loads.append(pltpu.make_async_copy(ins[i].at[at], bufs[i].at[at], got.at[s]))
        loads[-1].start()
    stores = []
    for s, (i, at) in enumerate(parts):
        loads[s].wait()
        stores.append(pltpu.make_async_copy(bufs[i].at[at], outs[i].at[at], put.at[s]))
        stores[-1].start()
    for cp in stores:
        cp.wait()


def finish(*arrays):
    hbm = pl.BlockSpec(memory_space=pl.ANY)
    return pl.pallas_call(
        finish_kernel,
        out_shape=tuple(jax.ShapeDtypeStruct(a.shape, a.dtype) for a in arrays),
        in_specs=[hbm] * 4,
        out_specs=(hbm,) * 4,
        scratch_shapes=[pltpu.VMEM(a.shape, a.dtype) for a in arrays]
        + [pltpu.SemaphoreType.DMA((16,)), pltpu.SemaphoreType.DMA((16,))],
        name="finish",
    )(*arrays)


def shards(tokens, cotangent, expert_ids, gate_weights, expert_weights, shared_weights):
    grad_tokens, grad_gates, grad_experts, grad_shared = layer(
        tokens, cotangent, expert_ids.T, gate_weights.T, expert_weights, shared_weights
    )
    grad_tokens, grad_gates, grad_experts, grad_shared = finish(
        grad_tokens, grad_gates, grad_experts, grad_shared
    )
    return (grad_tokens, grad_gates.T, grad_experts[None], grad_shared)


def solution(mesh):
    rows = P(("dp", "expert"), None)
    return jax.shard_map(
        shards,
        mesh=mesh,
        in_specs=(rows, rows, rows, rows, P(("dp", "expert"), None, None, None), P()),
        out_specs=(rows, rows, P(("dp", "expert"), None, None, None), P(None, "dp", None)),
        check_vma=False,
    )
```
